32 devices in a mesh: grp: 8 (over z, x), tp: 4 (over y, core).
Axes of the slice: x: 2, y: 2, z: 4, core: 2. Of those that a mesh axis runs over, the one named last changes fastest.
Arguments:
- q_nope: bfloat16 [512, 16384], P('grp', 'tp'), may hold values from -6 to 6
- q_rope: bfloat16 [512, 8192], P('grp', 'tp'), may hold values from -500 to 500
- w_uk: bfloat16 [128, 128, 512], P('tp'), may hold values from -0.5 to 0.5
- w_uv: bfloat16 [128, 512, 128], P('tp'), may hold values from -1 to 1
- prefix_latent: bfloat16 [16, 2048, 512], P('grp'), may hold values from -5 to 5
- prefix_rope: bfloat16 [16, 64, 2048], P('grp'), may hold values from -8 to 8
- suffix_latent: bfloat16 [512, 256, 512], P(('grp', 'tp')), may hold values from -5 to 5
- suffix_rope: bfloat16 [512, 64, 256], P(('grp', 'tp')), may hold values from -4 to 4
- suffix_len: int32 [8, 64], P('grp'), may hold values from 1 to 256, 8192 in all within a row
- request_prefix: int32 [512], P('grp'), may hold values from 0 to 15, as said below
- prefix_slot: int32 [16], replicated, may hold values from 0 to 15, as said below
Outputs:
- attended: bfloat16 [512, 16384], P('grp', 'tp')
The draws below stay inside these ranges and needn't reach their ends.
Inputs may be any that keep to these rules, and one draw needn't show every extreme that they name: `request_prefix`: of the requests of one group, at most 8 name the same prefix; in every draw one prefix is named by exactly 8 requests of every group. `prefix_slot`: A permutation: each cache row holds exactly one prefix. `suffix_len`: the lengths of one group sum to 8192, and one of them is 256.
All inputs are finite; a program needn't handle non-finite values.
Results may differ from the reference program's by a relative error of at most 0.018.
Values may be sent and summed in bfloat16 or wider, within the bound.
No kernel may reach another device: no remote copies, remote signals or barrier semaphores. Data moves between devices by JAX's collectives and lax.ppermute only.
A program may use at most 128 MiB of HBM per device.

```python
import math
import jax
import jax.numpy as jnp
import numpy as np
from jax import lax

HEADS = 128
LATENT = 512
ROPE_DIM = 64
NOPE_DIM = 128
VALUE_DIM = 128
REQ_DEV = 64
PLEN = 2048
SLEN = 256
GROUPS = 8
PREFIXES = 16
CAPP = 8
REQUESTS = 512


def route_draw(key):
    base_key = jax.random.fold_in(key, 101)
    hot_slot = jax.random.randint(jax.random.fold_in(base_key, 1), (), 0, PREFIXES)
    scores = jax.random.randint(jax.random.fold_in(base_key, 2), (GROUPS, PREFIXES * CAPP), 0, 1073741824)
    position = jnp.arange(PREFIXES * CAPP, dtype=jnp.int32)
    scores = jnp.where((position // CAPP)[None, :] == hot_slot, -1, scores)
    ranked = jnp.argsort(scores, axis=1, stable=True)[:, :REQ_DEV]
    shuffle_keys = jax.random.randint(jax.random.fold_in(base_key, 3), (GROUPS, REQ_DEV), 0, 1073741824)
    shuffle = jnp.argsort(shuffle_keys, axis=1, stable=True)
    chosen = jnp.take_along_axis(ranked, shuffle, axis=1)
    slot_ids = (chosen // CAPP).reshape(-1).astype(jnp.int32)
    permuted = jax.random.permutation(jax.random.fold_in(base_key, 4), PREFIXES).astype(jnp.int32)
    inverse = jnp.argsort(permuted).astype(jnp.int32)
    return (inverse[slot_ids], permuted)


def rope_table(key):
    drawn = jnp.clip(jax.random.normal(jax.random.fold_in(key, 202), (PREFIXES, ROPE_DIM, PLEN), jnp.float32), -4.0, 4.0)
    return drawn


def draw_request_prefix(key, part):
    return route_draw(key)[0]


def draw_prefix_slot(key, part):
    return route_draw(key)[1]


def draw_prefix_rope(key, part):
    return rope_table(key).astype(jnp.bfloat16)


def draw_q_rope(key, part):
    drawn = jnp.clip(jax.random.normal(jax.random.fold_in(key, 303), (REQUESTS, HEADS * ROPE_DIM), jnp.float32), -4.0, 4.0)
    return drawn.astype(jnp.bfloat16)


def shard_levels(key, dims, cuts, low, high):
    factor_of = 1.0
    for dim, parts in cuts:
        heights = jax.random.uniform(jax.random.fold_in(jax.random.fold_in(key, 6), dim), (parts,), jnp.float32, low / len(cuts), high / len(cuts))
        factor_of = factor_of * jnp.repeat(jnp.exp(heights), dims[dim] // parts).reshape((-1,) + (1,) * (len(dims) - 1 - dim))
    return factor_of


def length_profile(number_of, total, limit, skew):
    weights = [(1 << 20) // math.isqrt(standing ** skew) + 1 for standing in range(2, number_of + 1)]
    surplus, counts = total - limit - (number_of - 1), [1] * (number_of - 1)
    while surplus > 0:
        candidates = [i for i in range(number_of - 1) if counts[i] < limit]
        whole, budget = sum([weights[i] for i in candidates]), surplus
        for i in candidates:
            addition = min(limit - counts[i], max(1, budget * weights[i] // whole), surplus)
            counts[i] = counts[i] + addition
            surplus = surplus - addition
    return np.array([limit] + counts)


def uneven(stream_key, amount, total, limit, slope):
    if amount == 2:
        one = jax.random.randint(stream_key, (), max(1, total - limit), min(limit, total - 1) + 1)
        return jnp.stack([one, total - one])
    sizes = jnp.asarray(length_profile(amount, total, limit, slope), jnp.int32)
    couples = (amount - 1) // 2
    donor, receiver = sizes[1:1 + 2 * couples:2], sizes[2:2 + 2 * couples:2]
    slack = jnp.minimum(donor - 1, limit - receiver)
    shifted = jax.random.randint(jax.random.fold_in(stream_key, 1), (couples,), 0, 1 << 20) % (slack + 1)
    sizes = sizes.at[1:1 + 2 * couples:2].set(donor - shifted).at[2:2 + 2 * couples:2].set(receiver + shifted)
    return sizes[jax.random.permutation(jax.random.fold_in(stream_key, 2), amount)]


def normal_values(key, extent, spread, bound, pieces=(), kind=jnp.bfloat16):
    values = jax.random.normal(key, extent, jnp.float32) * spread
    if len(pieces) > 0:
        values = shard_levels(key, extent, pieces, -0.22, 0.18) * values
    return jnp.clip(values, min=-bound, max=bound).astype(kind)


def setup_inputs(seed: int = 0) -> dict:
    seeds = jax.random.split(jax.random.key(seed), 12)
    q_nope = normal_values(seeds[0], (REQUESTS, HEADS * NOPE_DIM), 1.25, 6.0, ((0, 8), (1, 4)))
    q_rope = draw_q_rope(jax.random.fold_in(seeds[11], 71), 0)
    w_uk = normal_values(seeds[2], (HEADS, NOPE_DIM, LATENT), NOPE_DIM ** -0.5, 0.5, ((0, 4),))
    w_uv = normal_values(seeds[3], (HEADS, LATENT, VALUE_DIM), (LATENT // 16) ** -0.5, 1.0, ((0, 4),))
    prefix_latent = normal_values(seeds[4], (PREFIXES, PLEN, LATENT), 1.0, 5.0, ((0, 8),))
    prefix_rope = draw_prefix_rope(jax.random.fold_in(seeds[11], 71), 0)
    suffix_latent = normal_values(seeds[6], (REQUESTS, SLEN, LATENT), 1.0, 5.0, ((0, 32),))
    suffix_rope = normal_values(seeds[7], (REQUESTS, ROPE_DIM, SLEN), 1.0, 4.0, ((0, 32),))
    suffix_len = jax.vmap(lambda own: uneven(own, REQ_DEV, REQ_DEV * SLEN // 2, SLEN, 2))(jax.random.split(seeds[8], GROUPS)).reshape((GROUPS, REQ_DEV)).astype(jnp.int32)
    request_prefix = draw_request_prefix(jax.random.fold_in(seeds[11], 71), 0)
    prefix_slot = draw_prefix_slot(jax.random.fold_in(seeds[11], 71), 0)
    return {"q_nope": q_nope, "q_rope": q_rope, "w_uk": w_uk, "w_uv": w_uv, "prefix_latent": prefix_latent, "prefix_rope": prefix_rope, "suffix_latent": suffix_latent, "suffix_rope": suffix_rope, "suffix_len": suffix_len, "request_prefix": request_prefix, "prefix_slot": prefix_slot}


def partial_attention(latent_q, rope_q, latent_rows, rope_cols, live_mask, score_scale):
    scores = jnp.dot(latent_q, latent_rows.T, preferred_element_type=jnp.float32)
    scores = (scores + jnp.dot(rope_q, rope_cols, preferred_element_type=jnp.float32)) * score_scale
    scores = jnp.where(live_mask[None, :], scores, jnp.float32(-1e+30))
    highest = lax.optimization_barrier(jnp.max(scores, axis=1, keepdims=True))
    exponent = jnp.where(live_mask[None, :], jnp.exp(scores - highest), jnp.float32(0.0))
    summed = lax.optimization_barrier(jnp.sum(exponent, axis=1))
    weights = exponent.astype(jnp.bfloat16)
    latent_out = (jnp.dot(weights, latent_rows, preferred_element_type=jnp.float32) / summed[:, None]).astype(jnp.bfloat16)
    return (latent_out, highest[:, 0], summed)

def reference(q_nope, q_rope, w_uk, w_uv, prefix_latent, prefix_rope, suffix_latent, suffix_rope, suffix_len, request_prefix, prefix_slot):
    score_scale = 1.0 / math.sqrt(NOPE_DIM + ROPE_DIM)
    slot_ids = prefix_slot[request_prefix].astype(jnp.int32)
    lengths = suffix_len.reshape(-1).astype(jnp.int32)
    nope_heads = q_nope.reshape(REQUESTS, HEADS, NOPE_DIM).astype(jnp.float32)
    q_latent = jnp.einsum('rhd,hdc->rhc', nope_heads, w_uk.astype(jnp.float32)).astype(jnp.bfloat16)
    rope_heads = q_rope.reshape(REQUESTS, HEADS, ROPE_DIM)
    w_uv_wide = w_uv.astype(jnp.float32)
    positions = jnp.arange(SLEN, dtype=jnp.int32)
    prefix_live = jnp.ones((PLEN,), dtype=bool)

    def one_request(request_items):
        latent_q, rope_q, slot_id, suffix_rows, suffix_cols, length = request_items
        latent_rows = lax.dynamic_index_in_dim(prefix_latent, slot_id, 0, keepdims=False)
        rope_cols = lax.dynamic_index_in_dim(prefix_rope, slot_id, 0, keepdims=False)
        prefix_out, prefix_max, prefix_total = partial_attention(latent_q, rope_q, latent_rows, rope_cols, prefix_live, score_scale)
        prefix_values = jnp.einsum('hc,hcv->hv', prefix_out.astype(jnp.float32), w_uv_wide).astype(jnp.bfloat16)
        suffix_live = positions < length
        suffix_out, suffix_max, suffix_total = partial_attention(latent_q, rope_q, suffix_rows, suffix_cols, suffix_live, score_scale)
        suffix_values = jnp.einsum('hc,hcv->hv', suffix_out.astype(jnp.float32), w_uv_wide).astype(jnp.bfloat16)
        overall = jnp.maximum(prefix_max, suffix_max)
        prefix_share = prefix_total * jnp.exp(prefix_max - overall)
        suffix_share = suffix_total * jnp.exp(suffix_max - overall)
        mixed = prefix_share[:, None] * prefix_values.astype(jnp.float32) + suffix_share[:, None] * suffix_values.astype(jnp.float32)
        mixed = mixed / (prefix_share + suffix_share)[:, None]
        return mixed.astype(jnp.bfloat16).reshape(-1)
    return lax.map(one_request, (q_latent, rope_heads, slot_ids, suffix_latent, suffix_rope, lengths))
```

```python
import functools
import math

import jax
import jax.numpy as jnp
from jax import lax
from jax.experimental import pallas as pl
from jax.experimental.pallas import tpu as pltpu
from jax.sharding import PartitionSpec as P

F32 = jnp.float32
BF16 = jnp.bfloat16
LANES = 128
NT = (((1,), (1,)), ((), ()))
TN = (((0,), (0,)), ((), ()))


def whole_spec(shape):
    return pl.BlockSpec(shape, lambda *_: (0,) * len(shape))


def params(*semantics):
    return pltpu.CompilerParams(dimension_semantics=semantics)


def send_body(ids, table, nope, rope, *outs, shards, capacity):
    prefixes = table.shape[0]
    requests = ids.shape[1]
    prefix_iota = lax.broadcasted_iota(jnp.int32, (prefixes, requests), 0)
    named = ids[...] == prefix_iota
    slot = jnp.sum(jnp.where(named, table[...], 0), axis=0, keepdims=True)
    hits = (slot == prefix_iota).astype(F32)
    before = lax.broadcasted_iota(jnp.int32, (requests, requests), 0) < lax.broadcasted_iota(
        jnp.int32, (requests, requests), 1
    )
    earlier = jnp.dot(hits, before.astype(F32), preferred_element_type=F32)
    rank = jnp.sum(earlier * hits, axis=0, keepdims=True).astype(jnp.int32)
    rows = outs[0].shape[0]
    row = lax.broadcasted_iota(jnp.int32, (rows, requests), 0)
    width = nope.shape[1]
    for w in range(shards):
        pick = (slot == (row // capacity) * shards + w) & (rank == row % capacity)
        sel = pick.astype(F32).astype(BF16)
        out = outs[w]
        out[:, 0:width] = jnp.dot(sel, nope[...], preferred_element_type=F32).astype(BF16)
        out[:, width : width + rope.shape[1]] = jnp.dot(
            sel, rope[...], preferred_element_type=F32
        ).astype(BF16)
        filled = jnp.sum(pick.astype(F32), axis=1, keepdims=True)
        out[:, width + rope.shape[1] :] = jnp.broadcast_to(filled, (rows, LANES)).astype(BF16)
        outs[shards + w][...] = sel


def make_send(ids, table, q_nope, q_rope, groups, shards, capacity):
    rows = groups * capacity
    requests = q_nope.shape[0]
    width = q_nope.shape[1] + q_rope.shape[1] + LANES
    shapes = [jax.ShapeDtypeStruct((rows, width), BF16)] * shards
    shapes += [jax.ShapeDtypeStruct((rows, requests), BF16)] * shards
    return pl.pallas_call(
        functools.partial(send_body, shards=shards, capacity=capacity),
        out_shape=shapes,
        cost_estimate=pl.CostEstimate(
            flops=2 * shards * rows * requests * width, bytes_accessed=2**22, transcendentals=0
        ),
    )(ids.reshape(1, requests), table.reshape(-1, 1), q_nope, q_rope)


def latent_body(me, nope, rope, w_uk, *refs, near, far, pieces, block):
    step = pl.program_id(0)
    steps = pl.num_programs(0)
    n_out = near + far * pieces
    q_outs, rope_outs = refs[:n_out], refs[n_out : n_out + near + far]
    q_all, rope_all = refs[n_out + near + far :]
    requests = nope.shape[0]
    width = w_uk.shape[1]
    heads = q_all.shape[1] // requests
    half = heads // 2
    for j in range(block):
        value = jnp.dot(
            nope[:, j * width : (j + 1) * width], w_uk[j], preferred_element_type=F32
        )
        place = (j % 2) * half + step * (block // 2) + j // 2
        for b in range(q_all.shape[0]):
            q_all[b, pl.ds(place, requests, stride=heads), :] = value[
                :, b * LANES : (b + 1) * LANES
            ]

    @pl.when(step == steps - 1)
    def _():
        for j in range(half):
            rope_all[pl.ds(j, requests, stride=half), :] = rope[
                :, j * LANES : (j + 1) * LANES
            ].astype(F32)
        share = requests // (near + far)
        for s in range(near + far):
            there = me[0] ^ s
            parts = 1 if s < near else pieces
            each = share // parts
            for piece in range(parts):
                ref = q_outs[s if s < near else near + (s - near) * pieces + piece]
                base = pl.multiple_of((there * share + piece * each) * heads, heads)
                for b in range(q_all.shape[0]):
                    part = q_all[b, pl.ds(base, each * heads), :].astype(BF16)
                    ref[:, :, b * LANES : (b + 1) * LANES] = part.reshape(each, heads, LANES)
            ref = rope_outs[s]
            base = pl.multiple_of(there * share * half, half)
            ref[...] = rope_all[pl.ds(base, share * half), :].astype(BF16).reshape(ref.shape)


def latent_queries(me, q_nope, q_rope, w_uk, near, far, pieces):
    requests = q_nope.shape[0]
    heads, width, latent = w_uk.shape
    block = 8
    share = requests // (near + far)
    each = share // pieces
    q_shapes = [(share, heads, latent)] * near + [(each, heads, latent)] * (far * pieces)
    rope_shapes = [(share, heads // 2, LANES)] * (near + far)
    shapes = q_shapes + rope_shapes
    return pl.pallas_call(
        functools.partial(latent_body, near=near, far=far, pieces=pieces, block=block),
        grid_spec=pltpu.PrefetchScalarGridSpec(
            num_scalar_prefetch=1,
            grid=(heads // block,),
            in_specs=[
                pl.BlockSpec((requests, block * width), lambda i, _: (0, i)),
                whole_spec(q_rope.shape),
                pl.BlockSpec((block, width, latent), lambda i, _: (i, 0, 0)),
            ],
            out_specs=[whole_spec(s) for s in shapes],
            scratch_shapes=[
                pltpu.VMEM((latent // LANES, requests * heads, LANES), F32),
                pltpu.VMEM((requests * heads // 2, LANES), F32),
            ],
        ),
        out_shape=[jax.ShapeDtypeStruct(s, BF16) for s in shapes],
        compiler_params=params("arbitrary"),
        cost_estimate=pl.CostEstimate(
            flops=4 * requests * heads * width * latent, bytes_accessed=2**23, transcendentals=0
        ),
    )(me, q_nope, q_rope, w_uk)


def suffix_body(where, lengths, *refs, sources, unroll, scale):
    step = pl.program_id(0)
    qs, ropes = refs[:sources], refs[sources : 2 * sources]
    cache, keys = refs[2 * sources : 2 * sources + 2]
    outs = refs[2 * sources + 2 : 3 * sources + 2]
    lse_out = refs[3 * sources + 2]
    heads = qs[0].shape[1]
    dims = keys.shape[1]
    tokens = cache.shape[1]
    half_lane = lax.broadcasted_iota(jnp.int32, (heads // 2, 2 * dims), 1)
    rows = sources * heads
    position = lax.broadcasted_iota(jnp.int32, (rows, tokens), 1)
    diag = lax.broadcasted_iota(jnp.int32, (rows, LANES), 0) == lax.broadcasted_iota(
        jnp.int32, (rows, LANES), 1
    )
    for u in range(unroll):
        query = jnp.concatenate([q[u] for q in qs], axis=0)
        parts = []
        for r in ropes:
            pair = r[u]
            zero = jnp.zeros_like(pair)
            parts.append(jnp.where(half_lane < dims, pair, zero))
            parts.append(jnp.where(half_lane < dims, zero, pair))
        rotary = jnp.concatenate(parts, axis=0)
        latent = cache[u]
        key = keys[u]
        both = jnp.concatenate([key, key], axis=0)
        scores = lax.dot_general(query, latent, NT, preferred_element_type=F32)
        scores = scores + jnp.dot(rotary, both, preferred_element_type=F32)
        length = lengths[where[0] + step * unroll + u]
        scores = jnp.where(position < length, scores, F32(-1e30))
        highest = jnp.max(scores, axis=1, keepdims=True)
        weights = jnp.exp2((scores - highest) * scale)
        summed = jnp.sum(weights, axis=1, keepdims=True)
        value = jnp.dot(weights.astype(BF16), latent, preferred_element_type=F32) / summed
        value = value.astype(BF16)
        for s in range(sources):
            outs[s][u] = value[s * heads : (s + 1) * heads]
        lse = highest * scale + jnp.log2(summed)
        lse_out[pl.ds(step * unroll + u, 1), :] = jnp.sum(
            jnp.where(diag, lse, F32(0.0)), axis=0, keepdims=True
        )


def suffix_attention(where, lengths, qs, ropes, cache, keys, first, scale):
    sources = len(qs)
    count, heads, latent = qs[0].shape
    unroll = min(4, count)
    tokens = cache.shape[1]
    dims = keys.shape[1]
    skip = first // unroll
    row_block = lambda i, *_: (i, 0, 0)
    part_block = lambda i, *_: (i + skip, 0, 0)
    out_shape = [jax.ShapeDtypeStruct(q.shape, BF16) for q in qs]
    out_shape.append(jax.ShapeDtypeStruct((count, LANES), F32))
    return pl.pallas_call(
        functools.partial(suffix_body, sources=sources, unroll=unroll, scale=scale),
        grid_spec=pltpu.PrefetchScalarGridSpec(
            num_scalar_prefetch=2,
            grid=(count // unroll,),
            in_specs=[pl.BlockSpec((unroll, heads, latent), row_block)] * sources
            + [pl.BlockSpec((unroll, heads // 2, 2 * dims), part_block)] * sources
            + [
                pl.BlockSpec((unroll, tokens, latent), part_block),
                pl.BlockSpec((unroll, dims, tokens), part_block),
            ],
            out_specs=[pl.BlockSpec((unroll, heads, latent), row_block)] * sources
            + [whole_spec((count, LANES))],
        ),
        out_shape=out_shape,
        compiler_params=params("arbitrary"),
        cost_estimate=pl.CostEstimate(
            flops=2 * sources * heads * count * tokens * (2 * latent + dims) * 4,
            bytes_accessed=2 * count * tokens * latent,
            transcendentals=sources * heads * count * tokens,
        ),
    )(where, lengths, *qs, *ropes, cache, keys)


def owner_body(nope, rope, w_uk, w_uv, latent, keys, out, query, both, *, block, scale):
    step = pl.program_id(0)
    rows = nope.shape[0]
    width, wide = w_uk.shape[1:]
    values = w_uv.shape[2]
    dims = keys.shape[0]
    tokens = latent.shape[0]
    heads = block * pl.num_programs(0)
    base = out.shape[1] - LANES

    @pl.when(step == 0)
    def _():
        both[0:dims, :] = keys[...]
        both[dims : 2 * dims, :] = keys[...]
        out[:, base:] = jnp.zeros((rows, LANES), BF16)

    lane = lax.broadcasted_iota(jnp.int32, (rows, 2 * dims), 1)
    for j in range(block):
        at = slice(j * rows, (j + 1) * rows)
        query[at, 0:wide] = jnp.dot(
            nope[:, j * width : (j + 1) * width], w_uk[j], preferred_element_type=F32
        ).astype(BF16)
        pair = rope[:, (j // 2) * 2 * dims : (j // 2 + 1) * 2 * dims]
        keep = (lane < dims) if j % 2 == 0 else (lane >= dims)
        query[at, wide:] = jnp.where(keep, pair, jnp.zeros_like(pair))
    piece = min(512, block * rows)
    chunk = 512
    for start in range(0, block * rows, piece):
        q_latent = query[start : start + piece, 0:wide]
        q_rotary = query[start : start + piece, wide:]
        scores = []
        for t in range(0, tokens, chunk):
            s = lax.dot_general(q_latent, latent[t : t + chunk, :], NT, preferred_element_type=F32)
            scores.append(
                s + jnp.dot(q_rotary, both[:, t : t + chunk], preferred_element_type=F32)
            )
        highest = functools.reduce(
            jnp.maximum, [jnp.max(s, axis=1, keepdims=True) for s in scores]
        )
        summed = None
        mixed = None
        for s, t in zip(scores, range(0, tokens, chunk)):
            weights = jnp.exp2((s - highest) * scale)
            part = jnp.sum(weights, axis=1, keepdims=True)
            product = jnp.dot(
                weights.astype(BF16), latent[t : t + chunk, :], preferred_element_type=F32
            )
            summed = part if summed is None else summed + part
            mixed = product if mixed is None else mixed + product
        mixed = (mixed / summed).astype(BF16)
        lse = highest * scale + jnp.log2(summed)
        column = lax.broadcasted_iota(jnp.int32, (rows, LANES), 1)
        for jj in range(piece // rows):
            j = start // rows + jj
            at = slice(jj * rows, (jj + 1) * rows)
            value = jnp.dot(mixed[at], w_uv[j], preferred_element_type=F32)
            head = step * block + j
            out[:, pl.ds(pl.multiple_of(head * values, LANES), values)] = value.astype(BF16)
            x = lse[at]
            top = x.astype(BF16).astype(F32)
            middle = (x - top).astype(BF16).astype(F32)
            low = x - top - middle
            old = out[:, base:].astype(F32)
            new = jnp.where(column == head, top, old)
            new = jnp.where(column == heads + head, middle, new)
            new = jnp.where(column == 2 * heads + head, low, new)
            out[:, base:] = new.astype(BF16)


def owner_attention(received, w_uk, w_uv, latent, keys, row, scale):
    rows = received.shape[0]
    heads, width, wide = w_uk.shape
    values = w_uv.shape[2]
    tokens = latent.shape[1]
    dims = keys.shape[1]
    block = 8
    rope_at = heads * width // (block * dims)
    return pl.pallas_call(
        functools.partial(owner_body, block=block, scale=scale),
        grid=(heads // block,),
        in_specs=[
            pl.BlockSpec((rows, block * width), lambda i: (0, i)),
            pl.BlockSpec((rows, block * dims), lambda i: (0, rope_at + i)),
            pl.BlockSpec((block, width, wide), lambda i: (i, 0, 0)),
            pl.BlockSpec((block, wide, values), lambda i: (i, 0, 0)),
            pl.BlockSpec((None, tokens, wide), lambda i: (row, 0, 0)),
            pl.BlockSpec((None, dims, tokens), lambda i: (row, 0, 0)),
        ],
        out_specs=whole_spec((rows, heads * values + LANES)),
        out_shape=jax.ShapeDtypeStruct((rows, heads * values + LANES), BF16),
        scratch_shapes=[
            pltpu.VMEM((block * rows, wide + 2 * dims), BF16),
            pltpu.VMEM((2 * dims, tokens), BF16),
        ],
        compiler_params=params("arbitrary"),
        cost_estimate=pl.CostEstimate(
            flops=2 * heads * rows * tokens * (2 * wide + dims) * 2,
            bytes_accessed=2**24,
            transcendentals=heads * rows * tokens,
        ),
    )(received, received, w_uk, w_uv, latent, keys)


def mix_body(me, *refs, shards, near, far, pieces, block):
    step = pl.program_id(0)
    take = lambda n: [refs_iter.pop(0) for _ in range(n)]
    refs_iter = list(refs)
    places, backs, tails = take(shards), take(shards), take(shards)
    outs_near, outs_far = take(near), take(far * pieces)
    lse_near, lse_far = take(near), take(far * pieces)
    w_uv, out, s_all, lse_all = take(4)
    heads = outs_near[0].shape[1]
    requests = lse_all.shape[0]
    share = requests // (near + far)
    half = heads // 2
    values = w_uv.shape[2]

    @pl.when(step == 0)
    def _():
        for s in range(near + far):
            there = me[0] ^ s
            parts = 1 if s < near else pieces
            each = share // parts
            for piece in range(parts):
                k = (s - near) * pieces + piece
                ref = outs_near[s] if s < near else outs_far[k]
                lse = lse_near[s] if s < near else lse_far[k]
                index = s if s < near else s - near
                first = there * share + piece * each
                for b in range(s_all.shape[0]):
                    part = ref[:, :, b * LANES : (b + 1) * LANES].astype(F32)
                    s_all[b, pl.ds(pl.multiple_of(first * heads, heads), each * heads), :] = (
                        part.reshape(each * heads, LANES)
                    )
                lse_all[pl.ds(pl.multiple_of(first, each), each), :] = pltpu.roll(
                    lse[...], (LANES - index * heads) % LANES, 1
                )

    tail = sum(
        lax.dot_general(p[...], t[...], TN, preferred_element_type=F32)
        for p, t in zip(places, tails)
    )
    prefix = sum(
        lax.dot_general(p[...], b[...], TN, preferred_element_type=F32)
        for p, b in zip(places, backs)
    )
    lane = lax.broadcasted_iota(jnp.int32, (requests, LANES), 1)
    lse_rows = lse_all[...]
    for j in range(block):
        head = step * block + j
        place = (j % 2) * half + step * (block // 2) + j // 2
        rows = jnp.concatenate(
            [
                s_all[b, pl.ds(place, requests, stride=heads), :].astype(BF16)
                for b in range(s_all.shape[0])
            ],
            axis=1,
        )
        suffix = jnp.dot(rows, w_uv[j], preferred_element_type=F32).astype(BF16).astype(F32)
        mine = (lane < 3 * heads) & (lane % heads == head)
        lse_p = jnp.sum(jnp.where(mine, tail, F32(0.0)), axis=1, keepdims=True)
        lse_s = jnp.sum(jnp.where(lane == place, lse_rows, F32(0.0)), axis=1, keepdims=True)
        overall = jnp.maximum(lse_p, lse_s)
        a = jnp.exp2(lse_p - overall)
        b = jnp.exp2(lse_s - overall)
        mixed = (a * prefix[:, j * values : (j + 1) * values] + b * suffix) / (a + b)
        out[:, j * values : (j + 1) * values] = mixed.astype(BF16)


def mix(me, places, backs, outs_near, outs_far, lse_near, lse_far, w_uv, pieces):
    shards = len(places)
    near, far = len(outs_near), len(outs_far) // pieces
    heads, wide, values = w_uv.shape
    requests = places[0].shape[1]
    rows = backs[0].shape[0]
    block = 8
    tail_at = heads * values // LANES
    whole = lambda arrays: [whole_spec(a.shape) for a in arrays]
    return pl.pallas_call(
        functools.partial(
            mix_body, shards=shards, near=near, far=far, pieces=pieces, block=block
        ),
        grid_spec=pltpu.PrefetchScalarGridSpec(
            num_scalar_prefetch=1,
            grid=(heads // block,),
            in_specs=whole(places)
            + [pl.BlockSpec((rows, block * values), lambda i, _: (0, i))] * shards
            + [pl.BlockSpec((rows, LANES), lambda i, _: (0, tail_at))] * shards
            + whole(outs_near)
            + whole(outs_far)
            + whole(lse_near)
            + whole(lse_far)
            + [pl.BlockSpec((block, wide, values), lambda i, _: (i, 0, 0))],
            out_specs=pl.BlockSpec((requests, block * values), lambda i, _: (0, i)),
            scratch_shapes=[
                pltpu.VMEM((wide // LANES, requests * heads, LANES), F32),
                pltpu.VMEM((requests, LANES), F32),
            ],
        ),
        out_shape=jax.ShapeDtypeStruct((requests, heads * values), BF16),
        compiler_params=params("arbitrary"),
        cost_estimate=pl.CostEstimate(
            flops=4 * requests * heads * wide * values, bytes_accessed=2**23, transcendentals=0
        ),
    )(
        me,
        *places,
        *backs,
        *backs,
        *outs_near,
        *outs_far,
        *lse_near,
        *lse_far,
        w_uv,
    )


def local(
    q_nope,
    q_rope,
    w_uk,
    w_uv,
    prefix_latent,
    prefix_rope,
    suffix_latent,
    suffix_rope,
    suffix_len,
    request_prefix,
    prefix_slot,
):
    groups = lax.axis_size("grp")
    ranks = lax.axis_size("tp")
    requests = q_nope.shape[0]
    prefixes = prefix_slot.shape[0]
    shards = prefix_latent.shape[0]
    capacity = max(2, 2 * requests // prefixes)
    scale = math.log2(math.e) / math.sqrt(w_uk.shape[1] + prefix_rope.shape[1])
    share = requests // ranks
    near = 2
    far = ranks - near
    pieces = 2
    me = lax.axis_index("tp").astype(jnp.int32).reshape(1)
    lengths = suffix_len.reshape(-1)

    def swap(x, s):
        return lax.ppermute(x, "tp", [(k, k ^ s) for k in range(ranks)])

    def exchange(x):
        return lax.all_to_all(x, "grp", split_axis=0, concat_axis=0, tiled=True)

    made = make_send(request_prefix, prefix_slot, q_nope, q_rope, groups, shards, capacity)
    sends, places = made[:shards], made[shards:]
    received = [exchange(x) for x in sends]

    made = latent_queries(me, q_nope, q_rope, w_uk, near, far, pieces)
    q_near = made[:near]
    q_far = made[near : near + far * pieces]
    rope_out = made[near + far * pieces :]
    q_near = [q_near[0]] + [swap(q_near[s], s) for s in range(1, near)]
    ropes = [rope_out[0]] + [swap(rope_out[s], s) for s in range(1, ranks)]
    q_far = [[swap(q_far[s * pieces + p], near + s) for s in range(far)] for p in range(pieces)]

    *outs_near, lse_near = suffix_attention(
        me * share, lengths, q_near, ropes[:near], suffix_latent, suffix_rope, 0, scale
    )
    outs_near = [outs_near[0]] + [swap(outs_near[s], s) for s in range(1, near)]
    lse_near = [lse_near] + [swap(lse_near, s) for s in range(1, near)]

    outs_far = [None] * (far * pieces)
    lse_far = [None] * (far * pieces)
    for p in range(pieces):
        first = p * (share // pieces)
        *outs, lse = suffix_attention(
            me * share + first,
            lengths,
            q_far[p],
            ropes[near:],
            suffix_latent,
            suffix_rope,
            first,
            scale,
        )
        for s in range(far):
            outs_far[s * pieces + p] = swap(outs[s], near + s)
            lse_far[s * pieces + p] = swap(lse, near + s)

    backs = [
        exchange(owner_attention(received[w], w_uk, w_uv, prefix_latent, prefix_rope, w, scale))
        for w in range(shards)
    ]
    return mix(me, places, backs, outs_near, outs_far, lse_near, lse_far, w_uv, pieces)


def solution(mesh):
    in_specs = (
        P("grp", "tp"),
        P("grp", "tp"),
        P("tp", None, None),
        P("tp", None, None),
        P("grp", None, None),
        P("grp", None, None),
        P(("grp", "tp"), None, None),
        P(("grp", "tp"), None, None),
        P("grp", None),
        P("grp"),
        P(),
    )
    return jax.shard_map(
        local, mesh=mesh, in_specs=in_specs, out_specs=P("grp", "tp"), check_vma=False
    )
```

```python
import functools
import math

import jax
import jax.numpy as jnp
from jax import lax
from jax.experimental import pallas as pl
from jax.experimental.pallas import tpu as pltpu
from jax.sharding import PartitionSpec as P


F32 = jnp.float32
BF16 = jnp.bfloat16
LANES = 128
NT = (((1,), (1,)), ((), ()))
TN = (((0,), (0,)), ((), ()))


def call(body, shapes, limit_mib, flops, scratch=(), scalars=(), far=(), args=()):
    spaces = [pltpu.SMEM] * len(scalars) + [pltpu.HBM] * len(far) + [pltpu.VMEM] * len(args)
    far = [pltpu.with_memory_space_constraint(x, pltpu.HBM) for x in far]
    return pl.pallas_call(
        body,
        in_specs=[pl.BlockSpec(memory_space=space) for space in spaces],
        out_specs=[pl.BlockSpec(memory_space=pltpu.VMEM)] * len(shapes),
        out_shape=[jax.ShapeDtypeStruct(*shape) for shape in shapes],
        scratch_shapes=list(scratch),
        compiler_params=pltpu.CompilerParams(vmem_limit_bytes=limit_mib * 2**20),
        cost_estimate=pl.CostEstimate(flops=flops, bytes_accessed=2**20, transcendentals=0),
    )(*scalars, *far, *args)


PARTS = 4


def fetch(source, target, sem):
    copy = pltpu.make_async_copy(source, target, sem)
    copy.start()
    return copy


class Stream:
    def __init__(self, source, target, sems, parts=PARTS, ahead=2):
        size = source.shape[0] // parts
        at = [pl.ds(k * size, size) for k in range(parts)]
        self.copies = [
            pltpu.make_async_copy(source.at[x], target.at[x], sems.at[k])
            for k, x in enumerate(at)
        ]
        self.size = size
        self.started = 0
        self.waited = 0
        self.start(ahead)

    def start(self, count):
        for copy in self.copies[self.started : self.started + count]:
            copy.start()
        self.started = min(len(self.copies), self.started + count)

    def need(self, upto):
        while self.waited * self.size < upto:
            self.copies[self.waited].wait()
            self.waited += 1
            self.start(1)


def three(x):
    top = x.astype(BF16).astype(F32)
    middle = (x - top).astype(BF16).astype(F32)
    return top, middle, x - top - middle


def joined(x, step):
    return x + pltpu.roll(x, LANES - step, 1) + pltpu.roll(x, LANES - 2 * step, 1)


def iota(shape, axis):
    return lax.broadcasted_iota(jnp.int32, shape, axis)


def send_body(me, table_far, ids_far, nope_far, rope_far, *refs, shards, capacity, apart):
    refs = list(refs)
    table, ids, nope, rope, sems = refs[-5:]
    pairs = ((table_far, table), (ids_far, ids), (nope_far, nope), (rope_far, rope))
    copies = [fetch(a, b, sems.at[k]) for k, (a, b) in enumerate(pairs)]
    copies[0].wait()
    copies[1].wait()
    prefixes = table.shape[0]
    requests = ids.shape[1]
    named = ids[...]
    slot = jnp.zeros((1, requests), jnp.int32)
    for p in range(prefixes):
        slot = slot + jnp.where(named == p, table[p], 0)
    hits = (slot == iota((prefixes, requests), 0)).astype(F32)
    before = iota((requests, requests), 0) < iota((requests, requests), 1)
    earlier = jnp.dot(hits, before.astype(F32), preferred_element_type=F32)
    rank = jnp.sum(earlier * hits, axis=0, keepdims=True).astype(jnp.int32)
    groups = prefixes // shards
    rows = groups * capacity
    row = iota((rows, requests), 0)
    width = nope.shape[1]
    copies[2].wait()
    copies[3].wait()
    for w in range(shards):
        owner = row // capacity
        if w in apart:
            owner = owner ^ me[0]
        pick = (slot == owner * shards + w) & (rank == row % capacity)
        sel = pick.astype(F32).astype(BF16)
        filled = jnp.sum(pick.astype(F32), axis=1, keepdims=True)
        parts = (
            (0, jnp.dot(sel, nope[...], preferred_element_type=F32)),
            (width, jnp.dot(sel, rope[...], preferred_element_type=F32)),
            (width + rope.shape[1], jnp.broadcast_to(filled, (rows, LANES))),
        )
        outs = [refs.pop(0) for _ in range(groups if w in apart else 1)]
        each = rows // len(outs)
        for k, out in enumerate(outs):
            for at, part in parts:
                out[:, at : at + part.shape[1]] = part[k * each : (k + 1) * each].astype(BF16)
        refs.pop(0)[...] = sel


def make_send(me, ids, table, q_nope, q_rope, groups, shards, capacity, apart):
    rows = groups * capacity
    requests = q_nope.shape[0]
    width = q_nope.shape[1] + q_rope.shape[1] + LANES
    counts = [groups if w in apart else 1 for w in range(shards)]
    shapes = []
    for count in counts:
        shapes += [((rows // count, width), BF16)] * count + [((rows, requests), BF16)]
    made = call(
        functools.partial(send_body, shards=shards, capacity=capacity, apart=apart),
        shapes,
        8,
        2 * shards * rows * requests * width,
        scratch=[
            pltpu.SMEM(table.shape, jnp.int32),
            pltpu.VMEM((1, requests), jnp.int32),
            pltpu.VMEM(q_nope.shape, BF16),
            pltpu.VMEM(q_rope.shape, BF16),
            pltpu.SemaphoreType.DMA((4,)),
        ],
        scalars=[me],
        far=[table, ids.reshape(1, requests), q_nope, q_rope],
    )
    made = list(made)
    sends, places = [], []
    for count in counts:
        sends.append([made.pop(0) for _ in range(count)])
        places.append(made.pop(0))
    return sends, places


def head_place(step, block, j, heads):
    return (j % 2) * (heads // 2) + step * (block // 2) + j // 2


def latent_body(me, nope_far, rope_far, w_uk_far, *refs, shares):
    outs = refs[: sum(shares)]
    q_all, rope_all, nope, rope, w_uk, sems = refs[sum(shares) :]
    copy_rope = fetch(rope_far, rope, sems.at[PARTS])
    copy_nope = fetch(nope_far, nope, sems.at[PARTS + 1])
    stream = Stream(w_uk_far, w_uk, sems)
    requests = nope.shape[0]
    heads, width, wide = w_uk.shape
    blocks = wide // LANES
    half = heads // 2
    copy_rope.wait()
    for j in range(half):
        rope_all[pl.ds(j, requests, stride=half), :] = rope[
            :, j * LANES : (j + 1) * LANES
        ].astype(F32)
    copy_nope.wait()
    for h in range(heads):
        stream.need(h + 1)
        value = jnp.dot(
            nope[:, h * width : (h + 1) * width], w_uk[h], preferred_element_type=F32
        )
        for b in range(blocks):
            q_all[b, pl.ds(head_place(0, heads, h, heads), requests, stride=heads), :] = value[
                :, b * LANES : (b + 1) * LANES
            ]
    share = requests // len(shares)
    outs = list(outs)
    for s, parts in enumerate(shares):
        there = me[0] ^ s
        each = share // parts
        some = each // blocks
        for piece in range(parts):
            ref = outs.pop(0)
            first = there * share + piece * each
            rows = each * heads
            for b in range(blocks):
                lanes = slice(b * LANES, (b + 1) * LANES)
                base = pl.multiple_of(first * heads, heads)
                ref[0:rows, lanes] = q_all[b, pl.ds(base, rows), :].astype(BF16)
                base = pl.multiple_of((first + b * some) * half, half)
                ref[rows:, lanes] = rope_all[pl.ds(base, some * half), :].astype(BF16)


def latent_queries(me, q_nope, q_rope, w_uk, shares):
    requests = q_nope.shape[0]
    heads, width, wide = w_uk.shape
    share = requests // len(shares)
    shapes = []
    for parts in shares:
        each = share // parts
        rows = each * heads + each * q_rope.shape[1] // wide
        shapes += [((rows, wide), BF16)] * parts
    return call(
        functools.partial(latent_body, shares=shares),
        shapes,
        14,
        4 * requests * heads * width * wide,
        scratch=[
            pltpu.VMEM((wide // LANES, requests * heads, LANES), F32),
            pltpu.VMEM((requests * heads // 2, LANES), F32),
            pltpu.VMEM(q_nope.shape, BF16),
            pltpu.VMEM(q_rope.shape, BF16),
            pltpu.VMEM(w_uk.shape, BF16),
            pltpu.SemaphoreType.DMA((PARTS + 2,)),
        ],
        scalars=[me],
        far=[q_nope, q_rope, w_uk],
    )


TAIL = 16


def suffix_body(me, lengths, cache_far, keys_far, *refs, sources, count, first, scale):
    asks, outs = refs[:sources], refs[sources : 2 * sources]
    cache, keys, lse_all, sems, sems_keys = refs[2 * sources :]
    wide = asks[0].shape[1]
    dims, tokens = keys.shape[1:]
    heads = asks[0].shape[0] * wide // (count * (wide + dims))
    half = heads // 2
    some = count // (wide // LANES)
    mine = pl.ds(first, count)
    unroll = math.gcd(8, count)
    parts = 2 * count // unroll
    stream_keys = Stream(keys_far.at[mine], keys, sems_keys, parts)
    stream = Stream(cache_far.at[mine], cache, sems, parts)
    share = cache_far.shape[0]
    half_lane = iota((half, 2 * dims), 1)
    rows = sources * heads
    position = iota((rows, tokens), 1)
    diag = iota((rows, LANES), 0) == iota((rows, LANES), 1)
    for step in range(count // unroll):
        at = [step * unroll + u for u in range(unroll)]
        scores = []
        for r in at:
            stream_keys.need(r + 1)
            stream.need(r + 1)
            query = jnp.concatenate([q[r * heads : (r + 1) * heads] for q in asks], axis=0)
            pairs = []
            for ref in asks:
                low = count * heads + (r % some) * half
                pair = ref[low : low + half, r // some * LANES : (r // some + 1) * LANES]
                zero = jnp.zeros_like(pair)
                pairs.append(jnp.where(half_lane < dims, pair, zero))
                pairs.append(jnp.where(half_lane < dims, zero, pair))
            rotary = jnp.concatenate(pairs, axis=0)
            key = keys[r]
            both = jnp.concatenate([key, key], axis=0)
            s = lax.dot_general(query, cache[r], NT, preferred_element_type=F32)
            s = s + jnp.dot(rotary, both, preferred_element_type=F32)
            length = lengths[me[0] * share + first + r]
            scores.append(jnp.where(position < length, s, F32(-1e30)))
        highest = [jnp.max(s, axis=1, keepdims=True) for s in scores]
        weights = [jnp.exp2((s - m) * scale) for s, m in zip(scores, highest)]
        summed = [jnp.sum(w, axis=1, keepdims=True) for w in weights]
        for r, w, m, total in zip(at, weights, highest, summed):
            value = jnp.dot(w.astype(BF16), cache[r], preferred_element_type=F32)
            value = (value * (1.0 / total)).astype(BF16)
            for s in range(sources):
                outs[s][r * heads : (r + 1) * heads, :] = value[s * heads : (s + 1) * heads]
            lse = m * scale + jnp.log2(total)
            lse_all[r : r + 1, :] = jnp.sum(
                jnp.where(diag, lse, F32(0.0)), axis=0, keepdims=True
            )
    if count < TAIL:
        lse_all[count:, :] = jnp.zeros((TAIL - count, LANES), F32)
    lane = iota((TAIL, LANES), 1)
    lse = lse_all[...]
    for s in range(sources):
        x = pltpu.roll(lse, (LANES - s * heads) % LANES, 1)
        top, middle, low = three(jnp.where(lane < heads, x, F32(0.0)))
        x = top + pltpu.roll(middle, heads, 1) + pltpu.roll(low, 2 * heads, 1)
        outs[s][count * heads :, 0:LANES] = x.astype(BF16)
        outs[s][count * heads :, LANES:] = jnp.zeros((TAIL, wide - LANES), BF16)


def suffix_attention(me, lengths, asks, cache, keys, heads, count, first, scale):
    sources = len(asks)
    tokens, wide = cache.shape[1:]
    dims = keys.shape[1]
    parts = 2 * count // math.gcd(8, count)
    return call(
        functools.partial(
            suffix_body, sources=sources, count=count, first=first, scale=scale
        ),
        [((count * heads + TAIL, wide), BF16)] * sources,
        12,
        2 * sources * heads * count * tokens * (2 * wide + dims) * 4,
        scratch=[
            pltpu.VMEM((count, tokens, wide), BF16),
            pltpu.VMEM((count, dims, tokens), BF16),
            pltpu.VMEM((TAIL, LANES), F32),
            pltpu.SemaphoreType.DMA((parts,)),
            pltpu.SemaphoreType.DMA((parts,)),
        ],
        scalars=[me, lengths],
        far=[cache, keys],
        args=asks,
    )


def owner_body(w_uk_far, w_uv_far, latent_far, keys_far, *refs, arrays, index, sizes, scale):
    pieces, outs = refs[:arrays], refs[arrays : 2 * arrays]
    received, packed, query, both, result, latent, w_uk, w_uv = refs[2 * arrays : -3]
    sems, sems_uk, sems_uv = refs[-3:]
    slots = received.shape[0]
    heads, width, wide = w_uk.shape
    values = w_uv.shape[2]
    dims, tokens = keys_far.shape[1:]
    base = heads * values
    rope_at = heads * width
    stream_uk = Stream(w_uk_far, w_uk, sems_uk, PARTS, 1)
    copies = [
        fetch(latent_far.at[index], latent, sems.at[0]),
        fetch(keys_far.at[index], both.at[0:dims], sems.at[1]),
        fetch(keys_far.at[index], both.at[dims : 2 * dims], sems.at[2]),
    ]
    each = slots // arrays
    for k, piece in enumerate(pieces):
        received[k * each : (k + 1) * each, :] = piece[...].astype(received.dtype)
    filled = received[:, rope_at + heads * dims : rope_at + heads * dims + 1].astype(F32)
    here, there = iota((slots, slots), 0), iota((slots, slots), 1)
    filled_row = jnp.sum(jnp.where(here == there, filled, F32(0.0)), axis=0, keepdims=True)
    ahead = jnp.sum(jnp.where(here < there, filled, F32(0.0)), axis=0, keepdims=True)
    move = jnp.where((here == ahead.astype(jnp.int32)) & (filled_row > 0.5), 1.0, 0.0)
    move = move.astype(BF16)
    count = jnp.sum(filled_row).astype(jnp.int32)
    packed[...] = jnp.dot(
        move,
        received[:, 0 : rope_at + heads * dims].astype(BF16),
        preferred_element_type=F32,
    ).astype(BF16)
    for copy in copies:
        copy.wait()
    stream_uk.start(PARTS)
    stream_uv = Stream(w_uv_far, w_uv, sems_uv, PARTS, PARTS)
    part = heads // PARTS

    def attend(rows):
        block = min(heads, 512 // rows // 2 * 2)
        while heads % block:
            block -= 2
        lane = iota((rows, 2 * dims), 1)
        column = iota((rows, LANES), 1)
        chunk = 512
        result[0:rows, base:] = jnp.zeros((rows, LANES), BF16)

        def arrive(copies, step):
            if block % part:
                for k in range(PARTS):
                    pl.when(step == 0)(copies[k].wait)
                return
            for k in range(PARTS):
                pl.when(step == k * part // block)(copies[k].wait)

        def some_heads(step, _):
            arrive(stream_uk.copies, step)
            for j in range(block):
                head = step * block + j
                at = slice(j * rows, (j + 1) * rows)
                nope = packed[0:rows, pl.ds(pl.multiple_of(head * width, LANES), width)]
                query[at, 0:wide] = jnp.dot(
                    nope, w_uk[head], preferred_element_type=F32
                ).astype(BF16)
                if j % 2 == 0:
                    pair_at = pl.multiple_of(rope_at + head * dims, LANES)
                    pair = packed[0:rows, pl.ds(pair_at, 2 * dims)]
                keep = (lane < dims) if j % 2 == 0 else (lane >= dims)
                query[at, wide:] = jnp.where(keep, pair, jnp.zeros_like(pair))
            q_latent = query[0 : block * rows, 0:wide]
            q_rotary = query[0 : block * rows, wide:]
            scores = []
            for t in range(0, tokens, chunk):
                s = lax.dot_general(
                    q_latent, latent[t : t + chunk, :], NT, preferred_element_type=F32
                )
                scores.append(
                    s + jnp.dot(q_rotary, both[:, t : t + chunk], preferred_element_type=F32)
                )
            highest = functools.reduce(
                jnp.maximum, [jnp.max(s, axis=1, keepdims=True) for s in scores]
            )
            summed = None
            mixed = None
            for s, t in zip(scores, range(0, tokens, chunk)):
                weights = jnp.exp2((s - highest) * scale)
                part = jnp.sum(weights, axis=1, keepdims=True)
                product = jnp.dot(
                    weights.astype(BF16),
                    latent[t : t + chunk, :],
                    preferred_element_type=F32,
                )
                summed = part if summed is None else summed + part
                mixed = product if mixed is None else mixed + product
            mixed = (mixed * (1.0 / summed)).astype(BF16)
            lse = highest * scale + jnp.log2(summed)
            tail = jnp.zeros((rows, LANES), F32)
            arrive(stream_uv.copies, step)
            for j in range(block):
                at = slice(j * rows, (j + 1) * rows)
                head = step * block + j
                value = jnp.dot(mixed[at], w_uv[head], preferred_element_type=F32)
                result[0:rows, pl.ds(pl.multiple_of(head * values, LANES), values)] = (
                    value.astype(BF16)
                )
                top, middle, low = three(lse[at])
                place = head_place(step, block, j, heads)
                tail = jnp.where(column == place, top, tail)
                tail = jnp.where(column == heads + place, middle, tail)
                tail = jnp.where(column == 2 * heads + place, low, tail)
            result[0:rows, base:] = (result[0:rows, base:].astype(F32) + tail).astype(BF16)
            return 0

        lax.fori_loop(0, heads // block, some_heads, 0)
        answer = lax.dot_general(
            move[0:rows], result[0:rows, :], TN, preferred_element_type=F32
        )
        for k, out in enumerate(outs):
            out[...] = answer[k * each : (k + 1) * each].astype(BF16)

    for low, high in zip((-1,) + sizes[:-1], sizes):
        pl.when((count > low) & (count <= high))(functools.partial(attend, high))


def owner_attention(received, w_uk, w_uv, latent, keys, index, scale):
    arrays = len(received)
    each = received[0].shape[0]
    slots = arrays * each
    heads, width, wide = w_uk.shape
    values = w_uv.shape[2]
    tokens = latent.shape[1]
    dims = keys.shape[1]
    sizes = {-(-(slots * part // 4) // 16) * 16 for part in (2, 3)}
    sizes = tuple(sorted(x for x in sizes if x < slots)) + (slots,)
    return call(
        functools.partial(owner_body, arrays=arrays, index=index, sizes=sizes, scale=scale),
        [((each, heads * values + LANES), BF16)] * arrays,
        34,
        2 * heads * slots * tokens * (2 * wide + dims),
        scratch=[
            pltpu.VMEM((slots, received[0].shape[1]), F32),
            pltpu.VMEM((slots, heads * (width + dims)), BF16),
            pltpu.VMEM((max(512, 2 * slots), wide + 2 * dims), BF16),
            pltpu.VMEM((2 * dims, tokens), BF16),
            pltpu.VMEM((slots, heads * values + LANES), BF16),
            pltpu.VMEM((tokens, wide), BF16),
            pltpu.VMEM(w_uk.shape, BF16),
            pltpu.VMEM(w_uv.shape, BF16),
            pltpu.SemaphoreType.DMA((3,)),
            pltpu.SemaphoreType.DMA((PARTS,)),
            pltpu.SemaphoreType.DMA((PARTS,)),
        ],
        far=[w_uk, w_uv, latent, keys],
        args=received,
    )


def project_body(me, w_uv_far, *refs, shares):
    tells = list(refs[: sum(shares)])
    out, lse_out, s_all, w_uv, sems = refs[sum(shares) :]
    stream = Stream(w_uv_far, w_uv, sems)
    heads, wide, values = w_uv.shape
    requests = out.shape[0]
    blocks = wide // LANES
    share = requests // len(shares)
    for s, parts in enumerate(shares):
        there = me[0] ^ s
        each = share // parts
        for piece in range(parts):
            ref = tells.pop(0)
            first = there * share + piece * each
            rows = each * heads
            base = pl.multiple_of(first * heads, heads)
            for b in range(blocks):
                part = ref[0:rows, b * LANES : (b + 1) * LANES].astype(F32)
                s_all[b, pl.ds(base, rows), :] = part
            lse = joined(ref[rows:, 0:LANES].astype(F32), heads)
            lse_out[pl.ds(pl.multiple_of(first, each), each), :] = lse[0:each]
    for h in range(heads):
        stream.need(h + 1)
        place = head_place(0, heads, h, heads)
        rows = [
            s_all[b, pl.ds(place, requests, stride=heads), :].astype(BF16) for b in range(blocks)
        ]
        value = jnp.dot(jnp.concatenate(rows, axis=1), w_uv[h], preferred_element_type=F32)
        out[:, h * values : (h + 1) * values] = value.astype(BF16)


def project(me, tells, w_uv, requests, shares):
    heads, wide, values = w_uv.shape
    return call(
        functools.partial(project_body, shares=shares),
        [((requests, heads * values), BF16), ((requests, LANES), F32)],
        14,
        4 * requests * heads * wide * values,
        scratch=[
            pltpu.VMEM((wide // LANES, requests * heads, LANES), F32),
            pltpu.VMEM(w_uv.shape, BF16),
            pltpu.SemaphoreType.DMA((PARTS,)),
        ],
        scalars=[me],
        far=[w_uv],
        args=tells,
    )


def mix_body(*refs, arrays, heads):
    refs = list(refs)
    places = [refs.pop(0) for _ in arrays]
    backs = [[refs.pop(0) for _ in range(n)] for n in arrays]
    suffix, lse_s, out = refs[:3]
    scratches = refs[3:]
    values = out.shape[1] // heads
    for parts, scratch in zip(backs, scratches):
        each = parts[0].shape[0]
        for k, part in enumerate(parts):
            scratch[k * each : (k + 1) * each, :] = part[...].astype(F32)

    def gather(lo, hi):
        found = [
            lax.dot_general(p[...], b[:, lo:hi].astype(BF16), TN, preferred_element_type=F32)
            for p, b in zip(places, scratches)
        ]
        return functools.reduce(jnp.add, found)

    lse_p = joined(gather(heads * values, heads * values + LANES), heads)
    lse_s = lse_s[...]
    overall = jnp.maximum(lse_p, lse_s)
    a = jnp.exp2(lse_p - overall)
    b = jnp.exp2(lse_s - overall)
    total = 1.0 / (a + b)
    a = a * total
    b = b * total
    some = 4
    for first in range(0, heads, some):
        prefix = gather(first * values, (first + some) * values)
        for h in range(first, first + some):
            place = head_place(0, heads, h, heads)
            at = slice(h * values, (h + 1) * values)
            mine = prefix[:, (h - first) * values : (h - first + 1) * values]
            mixed = (
                a[:, place : place + 1] * mine
                + b[:, place : place + 1] * suffix[:, at].astype(F32)
            )
            out[:, at] = mixed.astype(BF16)


def mix(places, backs, suffix, lse, heads):
    requests, width = suffix.shape
    arrays = tuple(len(parts) for parts in backs)
    rows = places[0].shape[0]
    return call(
        functools.partial(mix_body, arrays=arrays, heads=heads),
        [((requests, width), BF16)],
        8,
        2 * requests * rows * width,
        scratch=[pltpu.VMEM((rows, width + LANES), F32)] * len(arrays),
        args=[*places, *[x for parts in backs for x in parts], suffix, lse],
    )[0]


def local(
    q_nope,
    q_rope,
    w_uk,
    w_uv,
    prefix_latent,
    prefix_rope,
    suffix_latent,
    suffix_rope,
    suffix_len,
    request_prefix,
    prefix_slot,
):
    groups = lax.axis_size("grp")
    ranks = lax.axis_size("tp")
    requests = q_nope.shape[0]
    prefixes = prefix_slot.shape[0]
    shards = prefix_latent.shape[0]
    capacity = max(2, 2 * requests // prefixes)
    scale = math.log2(math.e) / math.sqrt(w_uk.shape[1] + prefix_rope.shape[1])
    share = requests // ranks
    heads = w_uk.shape[0]
    near, pieces = min(2, ranks), 2
    shares = (1,) * near + (pieces,) * (ranks - near)
    apart = (shards - 1,)
    mine = lax.axis_index("grp").astype(jnp.int32).reshape(1)
    me = lax.axis_index("tp").astype(jnp.int32).reshape(1)
    lengths = suffix_len.reshape(-1)

    def swap(x, s, axis, size):
        if s == 0:
            return x
        return lax.ppermute(x, axis, [(k, k ^ s) for k in range(size)])

    def exchange(xs):
        if len(xs) > 1:
            return [swap(x, s, "grp", groups) for s, x in enumerate(xs)]
        return [lax.all_to_all(xs[0], "grp", split_axis=0, concat_axis=0, tiled=True)]

    sends, places = make_send(
        mine, request_prefix, prefix_slot, q_nope, q_rope, groups, shards, capacity, apart
    )
    received = [exchange(x) for x in sends]

    made = list(latent_queries(me, q_nope, q_rope, w_uk, shares))
    asks = [
        [swap(made.pop(0), s, "tp", ranks) for _ in range(parts)]
        for s, parts in enumerate(shares)
    ]

    def attend(some, p, count):
        return suffix_attention(
            me,
            lengths,
            [asks[s][p] for s in some],
            suffix_latent,
            suffix_rope,
            heads,
            count,
            p * count,
            scale,
        )

    tells = [[None] * parts for parts in shares]
    for s, x in enumerate(attend(range(near), 0, share)):
        tells[s][0] = swap(x, s, "tp", ranks)
    for p in range(pieces):
        for s, x in enumerate(attend(range(near, ranks), p, share // pieces), near):
            tells[s][p] = swap(x, s, "tp", ranks)

    backs = []
    for w in range(shards):
        result = owner_attention(
            received[w], w_uk, w_uv, prefix_latent, prefix_rope, w, scale
        )
        backs.append(exchange(result))
    suffix, lse = project(me, [x for parts in tells for x in parts], w_uv, requests, shares)
    return mix(places, backs, suffix, lse, heads)


def solution(mesh):
    in_specs = (
        P("grp", "tp"),
        P("grp", "tp"),
        P("tp", None, None),
        P("tp", None, None),
        P("grp", None, None),
        P("grp", None, None),
        P(("grp", "tp"), None, None),
        P(("grp", "tp"), None, None),
        P("grp", None),
        P("grp"),
        P(),
    )

    return jax.shard_map(
        local, mesh=mesh, in_specs=in_specs, out_specs=P("grp", "tp"), check_vma=False
    )
```

```python
import functools
import math

import jax
import jax.numpy as jnp
from jax import lax
from jax.experimental import pallas as pl
from jax.experimental.pallas import tpu as pltpu
from jax.sharding import PartitionSpec as P


F32 = jnp.float32
BF16 = jnp.bfloat16
LANES = 128
NT = (((1,), (1,)), ((), ()))
TN = (((0,), (0,)), ((), ()))


def call(body, shapes, limit_mib, flops, scratch=(), scalars=(), far=(), args=()):
    spaces = [pltpu.SMEM] * len(scalars) + [pltpu.HBM] * len(far) + [pltpu.VMEM] * len(args)
    far = [pltpu.with_memory_space_constraint(x, pltpu.HBM) for x in far]
    return pl.pallas_call(
        body,
        in_specs=[pl.BlockSpec(memory_space=space) for space in spaces],
        out_specs=[pl.BlockSpec(memory_space=pltpu.VMEM)] * len(shapes),
        out_shape=[jax.ShapeDtypeStruct(*shape) for shape in shapes],
        scratch_shapes=list(scratch),
        compiler_params=pltpu.CompilerParams(vmem_limit_bytes=limit_mib * 2**20),
        cost_estimate=pl.CostEstimate(flops=flops, bytes_accessed=2**20, transcendentals=0),
    )(*scalars, *far, *args)


STRIDE = 40
PARTS = 4


def fetch(source, target, sem):
    copy = pltpu.make_async_copy(source, target, sem)
    copy.start()
    return copy


class Stream:
    def __init__(self, source, target, sems, parts=PARTS, ahead=2):
        size = source.shape[0] // parts
        at = [pl.ds(k * size, size) for k in range(parts)]
        self.copies = [
            pltpu.make_async_copy(source.at[x], target.at[x], sems.at[k])
            for k, x in enumerate(at)
        ]
        self.size = size
        self.started = 0
        self.waited = 0
        self.start(ahead)

    def start(self, count):
        for copy in self.copies[self.started : self.started + count]:
            copy.start()
        self.started = min(len(self.copies), self.started + count)

    def need(self, upto):
        while self.waited * self.size < upto:
            self.copies[self.waited].wait()
            self.waited += 1
            self.start(1)


def three(x):
    top = x.astype(BF16).astype(F32)
    middle = (x - top).astype(BF16).astype(F32)
    return top, middle, x - top - middle


def joined(x, step):
    return x + pltpu.roll(x, LANES - step, 1) + pltpu.roll(x, LANES - 2 * step, 1)


def iota(shape, axis):
    return lax.broadcasted_iota(jnp.int32, shape, axis)


def send_body(me, table_far, ids_far, nope_far, rope_far, *refs, shards, capacity, flips):
    refs = list(refs)
    table, ids, nope, rope, sems = refs[-5:]
    pairs = ((table_far, table), (ids_far, ids), (nope_far, nope), (rope_far, rope))
    copies = [fetch(a, b, sems.at[k]) for k, (a, b) in enumerate(pairs)]
    copies[0].wait()
    copies[1].wait()
    prefixes = table.shape[0]
    requests = ids.shape[1]
    named = ids[...]
    slot = jnp.zeros((1, requests), jnp.int32)
    for p in range(prefixes):
        slot = slot + jnp.where(named == p, table[p], 0)
    hits = (slot == iota((prefixes, requests), 0)).astype(F32)
    before = iota((requests, requests), 0) < iota((requests, requests), 1)
    earlier = jnp.dot(hits, before.astype(F32), preferred_element_type=F32)
    rank = jnp.sum(earlier * hits, axis=0, keepdims=True).astype(jnp.int32)
    each = shards * capacity
    count = prefixes // shards // len(flips)
    row = iota((count * each, requests), 0)
    width = nope.shape[1]
    copies[2].wait()
    copies[3].wait()
    for flip in flips:
        owner = (row // each * len(flips) + flip) ^ me[0]
        pick = (slot == owner * shards + row // capacity % shards) & (rank == row % capacity)
        sel = pick.astype(F32).astype(BF16)
        filled = jnp.sum(pick.astype(F32), axis=1, keepdims=True)
        parts = (
            (0, jnp.dot(sel, nope[...], preferred_element_type=F32)),
            (width, jnp.dot(sel, rope[...], preferred_element_type=F32)),
            (width + rope.shape[1], jnp.broadcast_to(filled, (count * each, LANES))),
        )
        for k in range(count):
            out = refs.pop(0)
            for at, part in parts:
                out[:, at : at + part.shape[1]] = part[k * each : (k + 1) * each].astype(BF16)
        refs.pop(0)[...] = sel


def make_send(me, ids, table, q_nope, q_rope, groups, shards, capacity, flips):
    requests = q_nope.shape[0]
    width = q_nope.shape[1] + q_rope.shape[1] + LANES
    each = shards * capacity
    count = groups // len(flips)
    shapes = ([((each, width), BF16)] * count + [((count * each, requests), BF16)]) * len(flips)
    made = call(
        functools.partial(send_body, shards=shards, capacity=capacity, flips=flips),
        shapes,
        8,
        2 * groups * each * requests * width,
        scratch=[
            pltpu.SMEM(table.shape, jnp.int32),
            pltpu.VMEM((1, requests), jnp.int32),
            pltpu.VMEM(q_nope.shape, BF16),
            pltpu.VMEM(q_rope.shape, BF16),
            pltpu.SemaphoreType.DMA((4,)),
        ],
        scalars=[me],
        far=[table, ids.reshape(1, requests), q_nope, q_rope],
    )
    made = [made[k * (count + 1) : (k + 1) * (count + 1)] for k in range(len(flips))]
    return [x[:count] for x in made], [x[count] for x in made]


def head_place(step, block, j, heads):
    return (j % 2) * (heads // 2) + step * (block // 2) + j // 2


def latent_body(me, nope_far, rope_far, w_uk_far, *refs, shares):
    outs = refs[: sum(shares)]
    q_all, rope_all, nope, rope, w_uk, sems = refs[sum(shares) :]
    copy_rope = fetch(rope_far, rope, sems.at[PARTS])
    copy_nope = fetch(nope_far, nope, sems.at[PARTS + 1])
    stream = Stream(w_uk_far, w_uk, sems)
    requests = nope.shape[0]
    heads, width, wide = w_uk.shape
    blocks = wide // LANES
    half = heads // 2
    copy_rope.wait()
    for j in range(half):
        rope_all[pl.ds(j, requests, stride=half), :] = rope[
            :, j * LANES : (j + 1) * LANES
        ].astype(F32)
    copy_nope.wait()
    for h in range(heads):
        stream.need(h + 1)
        value = jnp.dot(
            nope[:, h * width : (h + 1) * width], w_uk[h], preferred_element_type=F32
        )
        for b in range(blocks):
            q_all[b, pl.ds(head_place(0, heads, h, heads), requests, stride=STRIDE), :] = value[
                :, b * LANES : (b + 1) * LANES
            ]
    share = requests // len(shares)
    outs = list(outs)
    for s, parts in enumerate(shares):
        there = me[0] ^ s
        each = share // parts
        some = each // blocks
        for piece in range(parts):
            ref = outs.pop(0)
            first = there * share + piece * each
            rows = each * heads
            for b in range(blocks):
                lanes = slice(b * LANES, (b + 1) * LANES)
                for r in range(each):
                    base = pl.multiple_of((first + r) * STRIDE, 8)
                    ref[r * heads : (r + 1) * heads, lanes] = q_all[
                        b, pl.ds(base, heads), :
                    ].astype(BF16)
                base = pl.multiple_of((first + b * some) * half, half)
                ref[rows:, lanes] = rope_all[pl.ds(base, some * half), :].astype(BF16)


def latent_queries(me, q_nope, q_rope, w_uk, shares):
    requests = q_nope.shape[0]
    heads, width, wide = w_uk.shape
    share = requests // len(shares)
    shapes = []
    for parts in shares:
        each = share // parts
        rows = each * heads + each * q_rope.shape[1] // wide
        shapes += [((rows, wide), BF16)] * parts
    return call(
        functools.partial(latent_body, shares=shares),
        shapes,
        14,
        4 * requests * heads * width * wide,
        scratch=[
            pltpu.VMEM((wide // LANES, requests * STRIDE, LANES), F32),
            pltpu.VMEM((requests * heads // 2, LANES), F32),
            pltpu.VMEM(q_nope.shape, BF16),
            pltpu.VMEM(q_rope.shape, BF16),
            pltpu.VMEM(w_uk.shape, BF16),
            pltpu.SemaphoreType.DMA((PARTS + 2,)),
        ],
        scalars=[me],
        far=[q_nope, q_rope, w_uk],
    )


TAIL = 16


def suffix_body(me, lengths, cache, keys, *refs, sources, count, first, scale, resident):
    asks, outs = refs[:sources], refs[sources : 2 * sources]
    lse_all, *streamed = refs[2 * sources :]
    share = cache.shape[0]
    wide = asks[0].shape[1]
    dims, tokens = keys.shape[1:]
    heads = asks[0].shape[0] * wide // (count * (wide + dims))
    half = heads // 2
    some = count // (wide // LANES)
    mine = pl.ds(first, count)
    unroll = math.gcd(8, count)
    parts = 2 * count // unroll
    if not resident:
        cache_far, keys_far = cache, keys
        cache, keys, sems, sems_keys = streamed
        stream_keys = Stream(keys_far.at[mine], keys, sems_keys, parts, parts)
        stream = Stream(cache_far.at[mine], cache, sems, parts, parts)
    base = first if resident else 0
    half_lane = iota((half, 2 * dims), 1)
    rows = sources * heads
    position = iota((rows, tokens), 1)
    diag = iota((rows, LANES), 0) == iota((rows, LANES), 1)
    for step in range(count // unroll):
        at = [step * unroll + u for u in range(unroll)]
        scores = []
        for r in at:
            if not resident:
                stream_keys.need(r + 1)
                stream.need(r + 1)
            query = jnp.concatenate([q[r * heads : (r + 1) * heads] for q in asks], axis=0)
            pairs = []
            for ref in asks:
                low = count * heads + (r % some) * half
                pair = ref[low : low + half, r // some * LANES : (r // some + 1) * LANES]
                zero = jnp.zeros_like(pair)
                pairs.append(jnp.where(half_lane < dims, pair, zero))
                pairs.append(jnp.where(half_lane < dims, zero, pair))
            rotary = jnp.concatenate(pairs, axis=0)
            key = keys[base + r]
            both = jnp.concatenate([key, key], axis=0)
            s = lax.dot_general(query, cache[base + r], NT, preferred_element_type=F32)
            s = s + jnp.dot(rotary, both, preferred_element_type=F32)
            length = lengths[me[0] * share + first + r]
            scores.append(jnp.where(position < length, s, F32(-1e30)))
        highest = [jnp.max(s, axis=1, keepdims=True) for s in scores]
        weights = [jnp.exp2((s - m) * scale) for s, m in zip(scores, highest)]
        summed = [jnp.sum(w, axis=1, keepdims=True) for w in weights]
        for r, w, m, total in zip(at, weights, highest, summed):
            value = jnp.dot(w.astype(BF16), cache[base + r], preferred_element_type=F32)
            value = (value * (1.0 / total)).astype(BF16)
            for s in range(sources):
                outs[s][r * heads : (r + 1) * heads, :] = value[s * heads : (s + 1) * heads]
            lse = m * scale + jnp.log2(total)
            lse_all[r : r + 1, :] = jnp.sum(
                jnp.where(diag, lse, F32(0.0)), axis=0, keepdims=True
            )
    if count < TAIL:
        lse_all[count:, :] = jnp.zeros((TAIL - count, LANES), F32)
    lane = iota((TAIL, LANES), 1)
    lse = lse_all[...]
    for s in range(sources):
        x = pltpu.roll(lse, (LANES - s * heads) % LANES, 1)
        top, middle, low = three(jnp.where(lane < heads, x, F32(0.0)))
        x = top + pltpu.roll(middle, heads, 1) + pltpu.roll(low, 2 * heads, 1)
        outs[s][count * heads :, 0:LANES] = x.astype(BF16)
        outs[s][count * heads :, LANES:] = jnp.zeros((TAIL, wide - LANES), BF16)


def suffix_attention(me, lengths, asks, cache, keys, heads, count, first, scale, resident):
    sources = len(asks)
    tokens, wide = cache.shape[1:]
    dims = keys.shape[1]
    parts = 2 * count // math.gcd(8, count)
    scratch = [pltpu.VMEM((TAIL, LANES), F32)]
    if not resident:
        scratch += [
            pltpu.VMEM((count, tokens, wide), BF16),
            pltpu.VMEM((count, dims, tokens), BF16),
            pltpu.SemaphoreType.DMA((parts,)),
            pltpu.SemaphoreType.DMA((parts,)),
        ]
    return call(
        functools.partial(
            suffix_body,
            sources=sources,
            count=count,
            first=first,
            scale=scale,
            resident=resident,
        ),
        [((count * heads + TAIL, wide), BF16)] * sources,
        12,
        2 * sources * heads * count * tokens * (2 * wide + dims) * 4,
        scratch=scratch,
        scalars=[me, lengths],
        far=[] if resident else [cache, keys],
        args=[cache, keys, *asks] if resident else asks,
    )


def owner_body(w_uk, w_uv, latent, keys, *refs, arrays, capacity, sizes, scale):
    pieces, outs = refs[:arrays], refs[arrays : 2 * arrays]
    received, packed, query, both, result = refs[2 * arrays :]
    slots = received.shape[0]
    heads, width, wide = w_uk.shape
    values = w_uv.shape[2]
    shards, dims, tokens = keys.shape
    top_rows = slots // shards
    base = heads * values
    rope_at = heads * width
    both[:, 0:dims] = keys[...]
    both[:, dims:] = keys[...]
    each = slots // arrays
    for k, piece in enumerate(pieces):
        received[k * each : (k + 1) * each, :] = piece[...].astype(received.dtype)
    filled = received[:, rope_at + heads * dims : rope_at + heads * dims + 1].astype(F32)
    here, there = iota((slots, slots), 0), iota((slots, slots), 1)
    filled_row = jnp.sum(jnp.where(here == there, filled, F32(0.0)), axis=0, keepdims=True)
    shard_of = lambda x: x // capacity % shards
    alike = (here < there) & (shard_of(here) == shard_of(there))
    ahead = jnp.sum(jnp.where(alike, filled, F32(0.0)), axis=0, keepdims=True)
    goal = shard_of(there) * top_rows + ahead.astype(jnp.int32)
    move = jnp.where((here == goal) & (filled_row > 0.5), 1.0, 0.0).astype(BF16)
    row_shard = shard_of(iota((1, slots), 1))
    packed[...] = jnp.dot(
        move,
        received[:, 0 : rope_at + heads * dims].astype(BF16),
        preferred_element_type=F32,
    ).astype(BF16)
    result[...] = jnp.zeros(result.shape, BF16)

    def attend(w, rows):
        block = max(2, min(heads, 512 // rows // 2 * 2))
        while heads % block:
            block -= 2
        lane = iota((rows, 2 * dims), 1)
        column = iota((rows, LANES), 1)
        chunk = 512
        mine = pl.ds(pl.multiple_of(w * top_rows, top_rows), rows)

        def some_heads(step, _):
            for j in range(block):
                head = step * block + j
                at = slice(j * rows, (j + 1) * rows)
                nope = packed[mine, pl.ds(pl.multiple_of(head * width, LANES), width)]
                query[at, 0:wide] = jnp.dot(
                    nope, w_uk[head], preferred_element_type=F32
                ).astype(BF16)
                if j % 2 == 0:
                    pair_at = pl.multiple_of(rope_at + head * dims, LANES)
                    pair = packed[mine, pl.ds(pair_at, 2 * dims)]
                keep = (lane < dims) if j % 2 == 0 else (lane >= dims)
                query[at, wide:] = jnp.where(keep, pair, jnp.zeros_like(pair))

            q_latent = query[0 : block * rows, 0:wide]
            q_rotary = query[0 : block * rows, wide:]
            scores = []
            for t in range(0, tokens, chunk):
                s = lax.dot_general(
                    q_latent, latent[w, t : t + chunk, :], NT, preferred_element_type=F32
                )
                scores.append(
                    s + jnp.dot(q_rotary, both[w, :, t : t + chunk], preferred_element_type=F32)
                )
            highest = functools.reduce(
                jnp.maximum, [jnp.max(s, axis=1, keepdims=True) for s in scores]
            )
            summed = None
            mixed = None
            for s, t in zip(scores, range(0, tokens, chunk)):
                weights = jnp.exp2((s - highest) * scale)
                total = jnp.sum(weights, axis=1, keepdims=True)
                product = jnp.dot(
                    weights.astype(BF16), latent[w, t : t + chunk, :], preferred_element_type=F32
                )
                summed = total if summed is None else summed + total
                mixed = product if mixed is None else mixed + product
            mixed = (mixed * (1.0 / summed)).astype(BF16)
            lse = highest * scale + jnp.log2(summed)
            tail = jnp.zeros((rows, LANES), F32)
            for j in range(block):
                at = slice(j * rows, (j + 1) * rows)
                head = step * block + j
                value = jnp.dot(mixed[at], w_uv[head], preferred_element_type=F32)
                result[mine, pl.ds(pl.multiple_of(head * values, LANES), values)] = value.astype(
                    BF16
                )
                top, middle, low = three(lse[at])
                place = head_place(step, block, j, heads)
                tail = jnp.where(column == place, top, tail)
                tail = jnp.where(column == heads + place, middle, tail)
                tail = jnp.where(column == 2 * heads + place, low, tail)
            result[mine, base:] = (result[mine, base:].astype(F32) + tail).astype(BF16)
            return 0

        lax.fori_loop(0, heads // block, some_heads, 0)

    def one_shard(w, _):
        count = jnp.sum(jnp.where(row_shard == w, filled_row, F32(0.0))).astype(jnp.int32)
        for low, high in zip((-1,) + sizes[:-1], sizes):
            pl.when((count > low) & (count <= high))(functools.partial(attend, w, high))
        return 0

    lax.fori_loop(0, shards, one_shard, 0)
    answer = lax.dot_general(move, result[...], TN, preferred_element_type=F32)
    for k, out in enumerate(outs):
        out[...] = answer[k * each : (k + 1) * each].astype(BF16)


def owner_attention(received, w_uk, w_uv, latent, keys, capacity, scale):
    arrays = len(received)
    each = received[0].shape[0]
    slots = arrays * each
    heads, width, wide = w_uk.shape
    values = w_uv.shape[2]
    shards, tokens = latent.shape[:2]
    dims = keys.shape[1]
    top = slots // shards
    sizes = tuple(x for x in (16, 24) if x < top) + (top,)
    return call(
        functools.partial(
            owner_body, arrays=arrays, capacity=capacity, sizes=sizes, scale=scale
        ),
        [((each, heads * values + LANES), BF16)] * arrays,
        20,
        2 * heads * slots * tokens * (2 * wide + dims),
        scratch=[
            pltpu.VMEM((slots, received[0].shape[1]), BF16 if each % 16 == 0 else F32),
            pltpu.VMEM((slots, heads * (width + dims)), BF16),
            pltpu.VMEM((max(512, 2 * top), wide + 2 * dims), BF16),
            pltpu.VMEM((shards, 2 * dims, tokens), BF16),
            pltpu.VMEM((slots, heads * values + LANES), BF16),
        ],
        args=[w_uk, w_uv, latent, keys, *received],
    )


def project_body(me, w_uv, *refs, shares):
    tells = list(refs[: sum(shares)])
    out, lse_out, s_all = refs[sum(shares) :]
    heads, wide, values = w_uv.shape
    requests = out.shape[0]
    blocks = wide // LANES
    share = requests // len(shares)
    for s, parts in enumerate(shares):
        there = me[0] ^ s
        each = share // parts
        for piece in range(parts):
            ref = tells.pop(0)
            first = there * share + piece * each
            rows = each * heads
            for b in range(blocks):
                for r in range(each):
                    base = pl.multiple_of((first + r) * STRIDE, 8)
                    part = ref[r * heads : (r + 1) * heads, b * LANES : (b + 1) * LANES]
                    s_all[b, pl.ds(base, heads), :] = part.astype(F32)
            lse = joined(ref[rows:, 0:LANES].astype(F32), heads)
            lse_out[pl.ds(pl.multiple_of(first, each), each), :] = lse[0:each]
    for h in range(heads):
        place = head_place(0, heads, h, heads)
        rows = [
            s_all[b, pl.ds(place, requests, stride=STRIDE), :].astype(BF16) for b in range(blocks)
        ]
        value = jnp.dot(jnp.concatenate(rows, axis=1), w_uv[h], preferred_element_type=F32)
        out[:, h * values : (h + 1) * values] = value.astype(BF16)


def project(me, tells, w_uv, requests, shares):
    heads, wide, values = w_uv.shape
    return call(
        functools.partial(project_body, shares=shares),
        [((requests, heads * values), BF16), ((requests, LANES), F32)],
        14,
        4 * requests * heads * wide * values,
        scratch=[
            pltpu.VMEM((wide // LANES, requests * STRIDE, LANES), F32),
        ],
        scalars=[me],
        args=[w_uv, *tells],
    )


def mix_body(*refs, arrays, heads):
    refs = list(refs)
    places = [refs.pop(0) for _ in arrays]
    backs = [[refs.pop(0) for _ in range(n)] for n in arrays]
    suffix, lse_s, out = refs[:3]
    scratches = refs[3:]
    values = out.shape[1] // heads
    for parts, scratch in zip(backs, scratches):
        each = parts[0].shape[0]
        for k, part in enumerate(parts):
            scratch[k * each : (k + 1) * each, :] = part[...].astype(scratch.dtype)

    def gather(lo, hi):
        found = [
            lax.dot_general(p[...], b[:, lo:hi].astype(BF16), TN, preferred_element_type=F32)
            for p, b in zip(places, scratches)
        ]
        return functools.reduce(jnp.add, found)

    lse_p = joined(gather(heads * values, heads * values + LANES), heads)
    lse_s = lse_s[...]
    overall = jnp.maximum(lse_p, lse_s)
    a = jnp.exp2(lse_p - overall)
    b = jnp.exp2(lse_s - overall)
    total = 1.0 / (a + b)
    a = a * total
    b = b * total
    some = 4
    for first in range(0, heads, some):
        prefix = gather(first * values, (first + some) * values)
        for h in range(first, first + some):
            place = head_place(0, heads, h, heads)
            at = slice(h * values, (h + 1) * values)
            mine = prefix[:, (h - first) * values : (h - first + 1) * values]
            mixed = (
                a[:, place : place + 1] * mine
                + b[:, place : place + 1] * suffix[:, at].astype(F32)
            )
            out[:, at] = mixed.astype(BF16)


def mix(places, backs, suffix, lse, heads):
    requests, width = suffix.shape
    arrays = tuple(len(parts) for parts in backs)
    rows = places[0].shape[0]
    kind = BF16 if backs[0][0].shape[0] % 16 == 0 else F32
    return call(
        functools.partial(mix_body, arrays=arrays, heads=heads),
        [((requests, width), BF16)],
        8,
        2 * requests * rows * width,
        scratch=[pltpu.VMEM((rows, width + LANES), kind)] * len(arrays),
        args=[*places, *[x for parts in backs for x in parts], suffix, lse],
    )[0]


def local(
    q_nope,
    q_rope,
    w_uk,
    w_uv,
    prefix_latent,
    prefix_rope,
    suffix_latent,
    suffix_rope,
    suffix_len,
    request_prefix,
    prefix_slot,
):
    groups = lax.axis_size("grp")
    ranks = lax.axis_size("tp")
    requests = q_nope.shape[0]
    prefixes = prefix_slot.shape[0]
    shards = prefix_latent.shape[0]
    capacity = max(2, 2 * requests // prefixes)
    scale = math.log2(math.e) / math.sqrt(w_uk.shape[1] + prefix_rope.shape[1])
    share = requests // ranks
    heads = w_uk.shape[0]
    near, pieces = min(2, ranks), 1
    shares = (1,) * near + (pieces,) * (ranks - near)
    flips = tuple(range(min(2, groups)))
    mine = lax.axis_index("grp").astype(jnp.int32).reshape(1)
    me = lax.axis_index("tp").astype(jnp.int32).reshape(1)
    lengths = suffix_len.reshape(-1)

    def swap(x, s, axis, size):
        if s == 0:
            return x
        return lax.ppermute(x, axis, [(k, k ^ s) for k in range(size)])

    def exchange(xs, flip):
        last = len(flips)
        return [swap(x, d * last + flip, "grp", groups) for d, x in enumerate(xs)]

    sends, places = make_send(
        mine, request_prefix, prefix_slot, q_nope, q_rope, groups, shards, capacity, flips
    )
    order = flips
    received = {flip: exchange(sends[flip], flip) for flip in order}

    made = list(latent_queries(me, q_nope, q_rope, w_uk, shares))
    asks = [
        [swap(made.pop(0), s, "tp", ranks) for _ in range(parts)]
        for s, parts in enumerate(shares)
    ]

    def attend(some, p, count, resident):
        return suffix_attention(
            me,
            lengths,
            [asks[s][p] for s in some],
            suffix_latent,
            suffix_rope,
            heads,
            count,
            p * count,
            scale,
            resident,
        )

    tells = [[None] * parts for parts in shares]
    for s, x in enumerate(attend(range(near), 0, share, True)):
        tells[s][0] = swap(x, s, "tp", ranks)
    for p in range(pieces):
        for s, x in enumerate(attend(range(near, ranks), p, share // pieces, True), near):
            tells[s][p] = swap(x, s, "tp", ranks)

    backs = {}
    for flip in order:
        result = owner_attention(
            received[flip], w_uk, w_uv, prefix_latent, prefix_rope, capacity, scale
        )
        backs[flip] = exchange(result, flip)
    suffix, lse = project(me, [x for parts in tells for x in parts], w_uv, requests, shares)
    return mix(places, [backs[flip] for flip in flips], suffix, lse, heads)


def solution(mesh):
    in_specs = (
        P("grp", "tp"),
        P("grp", "tp"),
        P("tp", None, None),
        P("tp", None, None),
        P("grp", None, None),
        P("grp", None, None),
        P(("grp", "tp"), None, None),
        P(("grp", "tp"), None, None),
        P("grp", None),
        P("grp"),
        P(),
    )

    return jax.shard_map(
        local, mesh=mesh, in_specs=in_specs, out_specs=P("grp", "tp"), check_vma=False
    )
```

```python
import functools
import math

import jax
import jax.numpy as jnp
from jax import lax
from jax.experimental import pallas as pl
from jax.experimental.pallas import tpu as pltpu
from jax.sharding import PartitionSpec as P


F32 = jnp.float32
BF16 = jnp.bfloat16
LANES = 128
NT = (((1,), (1,)), ((), ()))
TN = (((0,), (0,)), ((), ()))


def call(body, shapes, limit_mib, flops, scratch=(), scalars=(), far=(), args=()):
    spaces = [pltpu.SMEM] * len(scalars) + [pltpu.HBM] * len(far) + [pltpu.VMEM] * len(args)
    far = [pltpu.with_memory_space_constraint(x, pltpu.HBM) for x in far]
    return pl.pallas_call(
        body,
        in_specs=[pl.BlockSpec(memory_space=space) for space in spaces],
        out_specs=[pl.BlockSpec(memory_space=pltpu.VMEM)] * len(shapes),
        out_shape=[jax.ShapeDtypeStruct(*shape) for shape in shapes],
        scratch_shapes=list(scratch),
        compiler_params=pltpu.CompilerParams(vmem_limit_bytes=limit_mib * 2**20),
        cost_estimate=pl.CostEstimate(flops=flops, bytes_accessed=2**20, transcendentals=0),
    )(*scalars, *far, *args)


STRIDE = 40
PARTS = 4


def fetch(source, target, sem):
    copy = pltpu.make_async_copy(source, target, sem)
    copy.start()
    return copy


class Stream:
    def __init__(self, source, target, sems, parts=PARTS, ahead=2):
        size = source.shape[0] // parts
        at = [pl.ds(k * size, size) for k in range(parts)]
        self.copies = [
            pltpu.make_async_copy(source.at[x], target.at[x], sems.at[k])
            for k, x in enumerate(at)
        ]
        self.size = size
        self.started = 0
        self.waited = 0
        self.start(ahead)

    def start(self, count):
        for copy in self.copies[self.started : self.started + count]:
            copy.start()
        self.started = min(len(self.copies), self.started + count)

    def need(self, upto):
        while self.waited * self.size < upto:
            self.copies[self.waited].wait()
            self.waited += 1
            self.start(1)


def three(x):
    top = x.astype(BF16).astype(F32)
    middle = (x - top).astype(BF16).astype(F32)
    return top, middle, x - top - middle


def joined(x, step):
    return x + pltpu.roll(x, LANES - step, 1) + pltpu.roll(x, LANES - 2 * step, 1)


def iota(shape, axis):
    return lax.broadcasted_iota(jnp.int32, shape, axis)


def send_body(me, table_far, ids_far, nope_far, rope_far, *refs, shards, capacity, flips):
    refs = list(refs)
    table, ids, nope, rope, sems = refs[-5:]
    pairs = ((table_far, table), (ids_far, ids), (nope_far, nope), (rope_far, rope))
    copies = [fetch(a, b, sems.at[k]) for k, (a, b) in enumerate(pairs)]
    copies[0].wait()
    copies[1].wait()
    prefixes = table.shape[0]
    requests = ids.shape[1]
    named = ids[...]
    slot = jnp.zeros((1, requests), jnp.int32)
    for p in range(prefixes):
        slot = slot + jnp.where(named == p, table[p], 0)
    hits = (slot == iota((prefixes, requests), 0)).astype(F32)
    before = iota((requests, requests), 0) < iota((requests, requests), 1)
    earlier = jnp.dot(hits, before.astype(F32), preferred_element_type=F32)
    rank = jnp.sum(earlier * hits, axis=0, keepdims=True).astype(jnp.int32)
    each = shards * capacity
    count = prefixes // shards // len(flips)
    row = iota((count * each, requests), 0)
    width = nope.shape[1]
    copies[2].wait()
    copies[3].wait()
    for flip in flips:
        owner = (row // each * len(flips) + flip) ^ me[0]
        pick = (slot == owner * shards + row // capacity % shards) & (rank == row % capacity)
        sel = pick.astype(F32).astype(BF16)
        filled = jnp.sum(pick.astype(F32), axis=1, keepdims=True)
        parts = (
            (0, jnp.dot(sel, nope[...], preferred_element_type=F32)),
            (width, jnp.dot(sel, rope[...], preferred_element_type=F32)),
            (width + rope.shape[1], jnp.broadcast_to(filled, (count * each, LANES))),
        )
        for k in range(count):
            out = refs.pop(0)
            for at, part in parts:
                out[:, at : at + part.shape[1]] = part[k * each : (k + 1) * each].astype(BF16)
        refs.pop(0)[...] = sel


def make_send(me, ids, table, q_nope, q_rope, groups, shards, capacity, flips):
    requests = q_nope.shape[0]
    width = q_nope.shape[1] + q_rope.shape[1] + LANES
    each = shards * capacity
    count = groups // len(flips)
    shapes = ([((each, width), BF16)] * count + [((count * each, requests), BF16)]) * len(flips)
    made = call(
        functools.partial(send_body, shards=shards, capacity=capacity, flips=flips),
        shapes,
        8,
        2 * groups * each * requests * width,
        scratch=[
            pltpu.SMEM(table.shape, jnp.int32),
            pltpu.VMEM((1, requests), jnp.int32),
            pltpu.VMEM(q_nope.shape, BF16),
            pltpu.VMEM(q_rope.shape, BF16),
            pltpu.SemaphoreType.DMA((4,)),
        ],
        scalars=[me],
        far=[table, ids.reshape(1, requests), q_nope, q_rope],
    )
    made = [made[k * (count + 1) : (k + 1) * (count + 1)] for k in range(len(flips))]
    return [x[:count] for x in made], [x[count] for x in made]


def head_place(step, block, j, heads):
    return (j % 2) * (heads // 2) + step * (block // 2) + j // 2


def latent_body(me, nope_far, rope_far, w_uk_far, *refs, shares):
    outs = refs[: sum(shares)]
    q_all, rope_all, nope, rope, w_uk, sems = refs[sum(shares) :]
    copy_rope = fetch(rope_far, rope, sems.at[PARTS])
    copy_nope = fetch(nope_far, nope, sems.at[PARTS + 1])
    stream = Stream(w_uk_far, w_uk, sems)
    requests = nope.shape[0]
    heads, width, wide = w_uk.shape
    blocks = wide // LANES
    half = heads // 2
    copy_rope.wait()
    for j in range(half):
        rope_all[pl.ds(j, requests, stride=half), :] = rope[
            :, j * LANES : (j + 1) * LANES
        ].astype(F32)
    copy_nope.wait()
    for h in range(heads):
        stream.need(h + 1)
        value = jnp.dot(
            nope[:, h * width : (h + 1) * width], w_uk[h], preferred_element_type=F32
        )
        for b in range(blocks):
            q_all[b, pl.ds(head_place(0, heads, h, heads), requests, stride=STRIDE), :] = value[
                :, b * LANES : (b + 1) * LANES
            ]
    share = requests // len(shares)
    outs = list(outs)
    for s, parts in enumerate(shares):
        there = me[0] ^ s
        each = share // parts
        some = each // blocks
        for piece in range(parts):
            ref = outs.pop(0)
            first = there * share + piece * each
            rows = each * heads
            for b in range(blocks):
                lanes = slice(b * LANES, (b + 1) * LANES)
                for r in range(each):
                    base = pl.multiple_of((first + r) * STRIDE, 8)
                    ref[r * heads : (r + 1) * heads, lanes] = q_all[
                        b, pl.ds(base, heads), :
                    ].astype(BF16)
                base = pl.multiple_of((first + b * some) * half, half)
                ref[rows:, lanes] = rope_all[pl.ds(base, some * half), :].astype(BF16)


def latent_queries(me, q_nope, q_rope, w_uk, shares):
    requests = q_nope.shape[0]
    heads, width, wide = w_uk.shape
    share = requests // len(shares)
    shapes = []
    for parts in shares:
        each = share // parts
        rows = each * heads + each * q_rope.shape[1] // wide
        shapes += [((rows, wide), BF16)] * parts
    return call(
        functools.partial(latent_body, shares=shares),
        shapes,
        14,
        4 * requests * heads * width * wide,
        scratch=[
            pltpu.VMEM((wide // LANES, requests * STRIDE, LANES), F32),
            pltpu.VMEM((requests * heads // 2, LANES), F32),
            pltpu.VMEM(q_nope.shape, BF16),
            pltpu.VMEM(q_rope.shape, BF16),
            pltpu.VMEM(w_uk.shape, BF16),
            pltpu.SemaphoreType.DMA((PARTS + 2,)),
        ],
        scalars=[me],
        far=[q_nope, q_rope, w_uk],
    )


TAIL = 16


def suffix_body(me, lengths, cache, keys, *refs, sources, count, first, scale, resident):
    asks, outs = refs[:sources], refs[sources : 2 * sources]
    lse_all, *streamed = refs[2 * sources :]
    share = cache.shape[0]
    wide = asks[0].shape[1]
    dims, tokens = keys.shape[1:]
    heads = asks[0].shape[0] * wide // (count * (wide + dims))
    half = heads // 2
    some = count // (wide // LANES)
    mine = pl.ds(first, count)
    unroll = math.gcd(8, count)
    parts = 2 * count // unroll
    if not resident:
        cache_far, keys_far = cache, keys
        cache, keys, sems, sems_keys = streamed
        stream_keys = Stream(keys_far.at[mine], keys, sems_keys, parts, parts)
        stream = Stream(cache_far.at[mine], cache, sems, parts, parts)
    base = first if resident else 0
    half_lane = iota((half, 2 * dims), 1)
    rows = sources * heads
    position = iota((rows, tokens), 1)
    diag = iota((rows, LANES), 0) == iota((rows, LANES), 1)
    for step in range(count // unroll):
        at = [step * unroll + u for u in range(unroll)]
        scores = []
        for r in at:
            if not resident:
                stream_keys.need(r + 1)
                stream.need(r + 1)
            query = jnp.concatenate([q[r * heads : (r + 1) * heads] for q in asks], axis=0)
            pairs = []
            for ref in asks:
                low = count * heads + (r % some) * half
                pair = ref[low : low + half, r // some * LANES : (r // some + 1) * LANES]
                zero = jnp.zeros_like(pair)
                pairs.append(jnp.where(half_lane < dims, pair, zero))
                pairs.append(jnp.where(half_lane < dims, zero, pair))
            rotary = jnp.concatenate(pairs, axis=0)
            key = keys[base + r]
            both = jnp.concatenate([key, key], axis=0)
            s = lax.dot_general(query, cache[base + r], NT, preferred_element_type=F32)
            s = s + jnp.dot(rotary, both, preferred_element_type=F32)
            length = lengths[me[0] * share + first + r]
            scores.append(jnp.where(position < length, s, F32(-1e30)))
        highest = [jnp.max(s, axis=1, keepdims=True) for s in scores]
        weights = [jnp.exp2((s - m) * scale) for s, m in zip(scores, highest)]
        summed = [jnp.sum(w, axis=1, keepdims=True) for w in weights]
        for r, w, m, total in zip(at, weights, highest, summed):
            value = jnp.dot(w.astype(BF16), cache[base + r], preferred_element_type=F32)
            value = (value * (1.0 / total)).astype(BF16)
            for s in range(sources):
                outs[s][r * heads : (r + 1) * heads, :] = value[s * heads : (s + 1) * heads]
            lse = m * scale + jnp.log2(total)
            lse_all[r : r + 1, :] = jnp.sum(
                jnp.where(diag, lse, F32(0.0)), axis=0, keepdims=True
            )
    if count < TAIL:
        lse_all[count:, :] = jnp.zeros((TAIL - count, LANES), F32)
    lane = iota((TAIL, LANES), 1)
    lse = lse_all[...]
    for s in range(sources):
        x = pltpu.roll(lse, (LANES - s * heads) % LANES, 1)
        top, middle, low = three(jnp.where(lane < heads, x, F32(0.0)))
        x = top + pltpu.roll(middle, heads, 1) + pltpu.roll(low, 2 * heads, 1)
        outs[s][count * heads :, 0:LANES] = x.astype(BF16)
        outs[s][count * heads :, LANES:] = jnp.zeros((TAIL, wide - LANES), BF16)


def suffix_attention(me, lengths, asks, cache, keys, heads, count, first, scale, resident):
    sources = len(asks)
    tokens, wide = cache.shape[1:]
    dims = keys.shape[1]
    parts = 2 * count // math.gcd(8, count)
    scratch = [pltpu.VMEM((TAIL, LANES), F32)]
    if not resident:
        scratch += [
            pltpu.VMEM((count, tokens, wide), BF16),
            pltpu.VMEM((count, dims, tokens), BF16),
            pltpu.SemaphoreType.DMA((parts,)),
            pltpu.SemaphoreType.DMA((parts,)),
        ]
    return call(
        functools.partial(
            suffix_body,
            sources=sources,
            count=count,
            first=first,
            scale=scale,
            resident=resident,
        ),
        [((count * heads + TAIL, wide), BF16)] * sources,
        12,
        2 * sources * heads * count * tokens * (2 * wide + dims) * 4,
        scratch=scratch,
        scalars=[me, lengths],
        far=[] if resident else [cache, keys],
        args=[cache, keys, *asks] if resident else asks,
    )


def owner_body(latent_far, w_uk, w_uv, keys, *refs, arrays, capacity, sizes, scale):
    pieces, outs = refs[:arrays], refs[arrays : 2 * arrays]
    received, packed, query, result, latent, sems = refs[2 * arrays :]
    stream = Stream(latent_far, latent, sems, latent.shape[0], latent.shape[0])
    slots = received.shape[0]
    heads, width, wide = w_uk.shape
    values = w_uv.shape[2]
    shards, dims, tokens = keys.shape
    top_rows = slots // shards
    base = heads * values
    rope_at = heads * width
    each = slots // arrays
    for k, piece in enumerate(pieces):
        received[k * each : (k + 1) * each, :] = piece[...].astype(received.dtype)
    filled = received[:, rope_at + heads * dims : rope_at + heads * dims + 1].astype(F32)
    here, there = iota((slots, slots), 0), iota((slots, slots), 1)
    filled_row = jnp.sum(jnp.where(here == there, filled, F32(0.0)), axis=0, keepdims=True)
    shard_of = lambda x: x // capacity % shards
    alike = (here < there) & (shard_of(here) == shard_of(there))
    ahead = jnp.sum(jnp.where(alike, filled, F32(0.0)), axis=0, keepdims=True)
    goal = shard_of(there) * top_rows + ahead.astype(jnp.int32)
    move = jnp.where((here == goal) & (filled_row > 0.5), 1.0, 0.0).astype(BF16)
    row_shard = shard_of(iota((1, slots), 1))
    packed[...] = jnp.dot(
        move,
        received[:, 0 : rope_at + heads * dims].astype(BF16),
        preferred_element_type=F32,
    ).astype(BF16)
    result[...] = jnp.zeros(result.shape, BF16)

    def attend(w, rows):
        block = max(2, min(heads, 512 // rows // 2 * 2))
        while heads % block:
            block -= 2
        column = iota((rows, LANES), 1)
        chunk = 256
        mine = pl.ds(pl.multiple_of(w * top_rows, top_rows), rows)

        def some_heads(step, _):
            for j in range(block):
                head = step * block + j
                at = slice(j * rows, (j + 1) * rows)
                nope = packed[mine, pl.ds(pl.multiple_of(head * width, LANES), width)]
                query[at, 0:wide] = jnp.dot(
                    nope, w_uk[head], preferred_element_type=F32
                ).astype(BF16)
                if j % 2 == 0:
                    pair_at = pl.multiple_of(rope_at + head * dims, LANES)
                    pair = packed[mine, pl.ds(pair_at, 2 * dims)]
                query[at, wide:] = pair[:, j % 2 * dims : (j % 2 + 1) * dims]
            for k, copy in enumerate(stream.copies):
                pl.when((w == k) & (step == 0))(copy.wait)
            q_latent = query[0 : block * rows, 0:wide]
            q_rotary = query[0 : block * rows, wide:]
            scores = []
            for t in range(0, tokens, chunk):
                s = lax.dot_general(
                    q_latent, latent[w, t : t + chunk, :], NT, preferred_element_type=F32
                )
                scores.append(
                    s + jnp.dot(q_rotary, keys[w, :, t : t + chunk], preferred_element_type=F32)
                )
            highest = functools.reduce(
                jnp.maximum, [jnp.max(s, axis=1, keepdims=True) for s in scores]
            )
            summed = None
            mixed = None
            for s, t in zip(scores, range(0, tokens, chunk)):
                weights = jnp.exp2((s - highest) * scale)
                total = jnp.sum(weights, axis=1, keepdims=True)
                product = jnp.dot(
                    weights.astype(BF16), latent[w, t : t + chunk, :], preferred_element_type=F32
                )
                summed = total if summed is None else summed + total
                mixed = product if mixed is None else mixed + product
            mixed = (mixed * (1.0 / summed)).astype(BF16)
            lse = highest * scale + jnp.log2(summed)
            tail = jnp.zeros((rows, LANES), F32)
            for j in range(block):
                at = slice(j * rows, (j + 1) * rows)
                head = step * block + j
                value = jnp.dot(mixed[at], w_uv[head], preferred_element_type=F32)
                result[mine, pl.ds(pl.multiple_of(head * values, LANES), values)] = value.astype(
                    BF16
                )
                top, middle, low = three(lse[at])
                place = head_place(step, block, j, heads)
                tail = jnp.where(column == place, top, tail)
                tail = jnp.where(column == heads + place, middle, tail)
                tail = jnp.where(column == 2 * heads + place, low, tail)
            result[mine, base:] = (result[mine, base:].astype(F32) + tail).astype(BF16)
            return 0

        lax.fori_loop(0, heads // block, some_heads, 0)

    def one_shard(w, _):
        count = jnp.sum(jnp.where(row_shard == w, filled_row, F32(0.0))).astype(jnp.int32)
        for low, high in zip((-1,) + sizes[:-1], sizes):
            pl.when((count > low) & (count <= high))(functools.partial(attend, w, high))
        return 0

    lax.fori_loop(0, shards, one_shard, 0)
    answer = lax.dot_general(move, result[...], TN, preferred_element_type=F32)
    for k, out in enumerate(outs):
        out[...] = answer[k * each : (k + 1) * each].astype(BF16)


def owner_attention(received, w_uk, w_uv, latent, keys, capacity, scale):
    arrays = len(received)
    each = received[0].shape[0]
    slots = arrays * each
    heads, width, wide = w_uk.shape
    values = w_uv.shape[2]
    shards, tokens = latent.shape[:2]
    dims = keys.shape[1]
    top = slots // shards
    sizes = tuple(x for x in (16, 24) if x < top) + (top,)
    return call(
        functools.partial(
            owner_body, arrays=arrays, capacity=capacity, sizes=sizes, scale=scale
        ),
        [((each, heads * values + LANES), BF16)] * arrays,
        24,
        2 * heads * slots * tokens * (2 * wide + dims),
        scratch=[
            pltpu.VMEM((slots, received[0].shape[1]), BF16 if each % 16 == 0 else F32),
            pltpu.VMEM((slots, heads * (width + dims)), BF16),
            pltpu.VMEM((max(512, 2 * top), wide + dims), BF16),
            pltpu.VMEM((slots, heads * values + LANES), BF16),
            pltpu.VMEM(latent.shape, BF16),
            pltpu.SemaphoreType.DMA((shards,)),
        ],
        far=[latent],
        args=[w_uk, w_uv, keys, *received],
    )


def project_body(me, w_uv, *refs, shares):
    tells = list(refs[: sum(shares)])
    out, lse_out, s_all = refs[sum(shares) :]
    heads, wide, values = w_uv.shape
    requests = out.shape[0]
    blocks = wide // LANES
    share = requests // len(shares)
    for s, parts in enumerate(shares):
        there = me[0] ^ s
        each = share // parts
        for piece in range(parts):
            ref = tells.pop(0)
            first = there * share + piece * each
            rows = each * heads
            for b in range(blocks):
                for r in range(each):
                    base = pl.multiple_of((first + r) * STRIDE, 8)
                    part = ref[r * heads : (r + 1) * heads, b * LANES : (b + 1) * LANES]
                    s_all[b, pl.ds(base, heads), :] = part.astype(F32)
            lse = joined(ref[rows:, 0:LANES].astype(F32), heads)
            lse_out[pl.ds(pl.multiple_of(first, each), each), :] = lse[0:each]
    for h in range(heads):
        place = head_place(0, heads, h, heads)
        rows = [
            s_all[b, pl.ds(place, requests, stride=STRIDE), :].astype(BF16) for b in range(blocks)
        ]
        value = jnp.dot(jnp.concatenate(rows, axis=1), w_uv[h], preferred_element_type=F32)
        out[:, h * values : (h + 1) * values] = value.astype(BF16)


def project(me, tells, w_uv, requests, shares):
    heads, wide, values = w_uv.shape
    return call(
        functools.partial(project_body, shares=shares),
        [((requests, heads * values), BF16), ((requests, LANES), F32)],
        14,
        4 * requests * heads * wide * values,
        scratch=[
            pltpu.VMEM((wide // LANES, requests * STRIDE, LANES), F32),
        ],
        scalars=[me],
        args=[w_uv, *tells],
    )


def mix_body(*refs, arrays, heads):
    refs = list(refs)
    places = [refs.pop(0) for _ in arrays]
    backs = [[refs.pop(0) for _ in range(n)] for n in arrays]
    suffix, lse_s, out = refs[:3]
    scratches = refs[3:]
    values = out.shape[1] // heads
    for parts, scratch in zip(backs, scratches):
        each = parts[0].shape[0]
        for k, part in enumerate(parts):
            scratch[k * each : (k + 1) * each, :] = part[...].astype(scratch.dtype)

    def gather(lo, hi):
        found = [
            lax.dot_general(p[...], b[:, lo:hi].astype(BF16), TN, preferred_element_type=F32)
            for p, b in zip(places, scratches)
        ]
        return functools.reduce(jnp.add, found)

    lse_p = joined(gather(heads * values, heads * values + LANES), heads)
    lse_s = lse_s[...]
    overall = jnp.maximum(lse_p, lse_s)
    a = jnp.exp2(lse_p - overall)
    b = jnp.exp2(lse_s - overall)
    total = 1.0 / (a + b)
    a = a * total
    b = b * total
    some = 4
    for first in range(0, heads, some):
        prefix = gather(first * values, (first + some) * values)
        for h in range(first, first + some):
            place = head_place(0, heads, h, heads)
            at = slice(h * values, (h + 1) * values)
            mine = prefix[:, (h - first) * values : (h - first + 1) * values]
            mixed = (
                a[:, place : place + 1] * mine
                + b[:, place : place + 1] * suffix[:, at].astype(F32)
            )
            out[:, at] = mixed.astype(BF16)


def mix(places, backs, suffix, lse, heads):
    requests, width = suffix.shape
    arrays = tuple(len(parts) for parts in backs)
    rows = places[0].shape[0]
    kind = BF16 if backs[0][0].shape[0] % 16 == 0 else F32
    return call(
        functools.partial(mix_body, arrays=arrays, heads=heads),
        [((requests, width), BF16)],
        8,
        2 * requests * rows * width,
        scratch=[pltpu.VMEM((rows, width + LANES), kind)] * len(arrays),
        args=[*places, *[x for parts in backs for x in parts], suffix, lse],
    )[0]


def local(
    q_nope,
    q_rope,
    w_uk,
    w_uv,
    prefix_latent,
    prefix_rope,
    suffix_latent,
    suffix_rope,
    suffix_len,
    request_prefix,
    prefix_slot,
):
    groups = lax.axis_size("grp")
    ranks = lax.axis_size("tp")
    requests = q_nope.shape[0]
    prefixes = prefix_slot.shape[0]
    shards = prefix_latent.shape[0]
    capacity = max(2, 2 * requests // prefixes)
    scale = math.log2(math.e) / math.sqrt(w_uk.shape[1] + prefix_rope.shape[1])
    share = requests // ranks
    heads = w_uk.shape[0]
    near, pieces = min(2, ranks), 1
    shares = (1,) * near + (pieces,) * (ranks - near)
    flips = tuple(range(min(2, groups)))
    mine = lax.axis_index("grp").astype(jnp.int32).reshape(1)
    me = lax.axis_index("tp").astype(jnp.int32).reshape(1)
    lengths = suffix_len.reshape(-1)

    def swap(x, s, axis, size):
        if s == 0:
            return x
        return lax.ppermute(x, axis, [(k, k ^ s) for k in range(size)])

    def exchange(xs, flip):
        last = len(flips)
        return [swap(x, d * last + flip, "grp", groups) for d, x in enumerate(xs)]

    sends, places = make_send(
        mine, request_prefix, prefix_slot, q_nope, q_rope, groups, shards, capacity, flips
    )
    order = flips
    received = {flip: exchange(sends[flip], flip) for flip in order}

    made = list(latent_queries(me, q_nope, q_rope, w_uk, shares))
    asks = [
        [swap(made.pop(0), s, "tp", ranks) for _ in range(parts)]
        for s, parts in enumerate(shares)
    ]

    def attend(some, p, count, resident):
        return suffix_attention(
            me,
            lengths,
            [asks[s][p] for s in some],
            suffix_latent,
            suffix_rope,
            heads,
            count,
            p * count,
            scale,
            resident,
        )

    tells = [[None] * parts for parts in shares]
    for s, x in enumerate(attend(range(near), 0, share, True)):
        tells[s][0] = swap(x, s, "tp", ranks)
    for p in range(pieces):
        for s, x in enumerate(attend(range(near, ranks), p, share // pieces, True), near):
            tells[s][p] = swap(x, s, "tp", ranks)

    backs = {}
    for flip in order:
        result = owner_attention(
            received[flip], w_uk, w_uv, prefix_latent, prefix_rope, capacity, scale
        )
        backs[flip] = exchange(result, flip)
    suffix, lse = project(me, [x for parts in tells for x in parts], w_uv, requests, shares)
    return mix(places, [backs[flip] for flip in flips], suffix, lse, heads)


def solution(mesh):
    in_specs = (
        P("grp", "tp"),
        P("grp", "tp"),
        P("tp", None, None),
        P("tp", None, None),
        P("grp", None, None),
        P("grp", None, None),
        P(("grp", "tp"), None, None),
        P(("grp", "tp"), None, None),
        P("grp", None),
        P("grp"),
        P(),
    )

    return jax.shard_map(
        local, mesh=mesh, in_specs=in_specs, out_specs=P("grp", "tp"), check_vma=False
    )
```
